32 devices in a mesh: row: 4 (over x, core), col: 8 (over z, y).
Axes of the slice: x: 2, y: 2, z: 4, core: 2. Of those that a mesh axis runs over, the one named last changes fastest.
Arguments:
- images: bfloat16 [128, 28, 28, 512], P(('row', 'col')), may hold values from -30 to 30
- w_reduce: bfloat16 [2, 512, 128], replicated, may hold values from -0.25 to 0.25
- w_spatial: bfloat16 [2, 3, 3, 128, 128], replicated, may hold values from -0.1875 to 0.1875
- w_expand: bfloat16 [2, 128, 512], replicated, may hold values from -0.5 to 0.5
- gain_mid: float32 [2, 2, 128], replicated, may hold values from 0.5 to 1.5
- bias_mid: float32 [2, 2, 128], replicated, may hold values from -3 to 3
- mean_mid: float32 [2, 2, 128], replicated, may hold values from -2 to 2
- var_mid: float32 [2, 2, 128], replicated, may hold values from 0.05 to 20
- gain_out: float32 [2, 512], replicated, may hold values from 0.5 to 1.5
- bias_out: float32 [2, 512], replicated, may hold values from -3 to 3
- mean_out: float32 [2, 512], replicated, may hold values from -2 to 2
- var_out: float32 [2, 512], replicated, may hold values from 0.05 to 20
Outputs:
- features: bfloat16 [128, 28, 28, 512], P(('row', 'col'))
The draws below stay inside these ranges and needn't reach their ends.
All inputs are finite; a program needn't handle non-finite values.
Results may differ from the reference program's by a relative error of at most 0.0075.
Values sent between devices are 32-bit elements; how exact they have to be, the bound alone decides.
A program may use at most 64 MiB of HBM per device.

```python
import math
import jax
import jax.numpy as jnp
from jax import lax

CIN = 512
MID = 128
SIDE = 28
BLOCKS = 2
IMAGES = 128


def draw_images(key, part):
    noise_key = jax.random.fold_in(key, 11)
    offset_key = jax.random.fold_in(key, 12)
    position = jnp.arange(IMAGES, dtype=jnp.float32) / max(IMAGES - 1, 1)
    offsets = 0.7 * jax.random.normal(offset_key, (IMAGES, 1, 1, CIN), jnp.float32)
    noise = jnp.clip(jax.random.normal(noise_key, (IMAGES, SIDE, SIDE, CIN), jnp.float32), -5.0, 5.0)
    scale = jnp.power(3.0, position)
    values = scale[:, None, None, None] * (noise + offsets)
    return jnp.clip(values, -30.0, 30.0).astype(jnp.bfloat16)


def normal_values(rng, dims, spread, reach, kind=jnp.bfloat16):
    return jnp.clip(spread * jax.random.normal(rng, dims, jnp.float32), -reach, reach).astype(kind)


def setup_inputs(seed: int = 0) -> dict:
    splits = jax.random.split(jax.random.key(seed), 13)
    return {
        "images": draw_images(jax.random.fold_in(splits[12], 71), 0),
        "w_reduce": normal_values(splits[1], (BLOCKS, CIN, MID), CIN ** -0.5, 0.25),
        "w_spatial": normal_values(splits[2], (BLOCKS, 3, 3, MID, MID), (9 * MID) ** -0.5, 0.1875),
        "w_expand": normal_values(splits[3], (BLOCKS, MID, CIN), MID ** -0.5, 0.5),
        "gain_mid": jnp.clip(1.0 + 0.1 * jax.random.normal(splits[4], (BLOCKS, 2, MID), jnp.float32), 0.5, 1.5),
        "bias_mid": normal_values(splits[5], (BLOCKS, 2, MID), 0.5, 3.0, jnp.float32),
        "mean_mid": jnp.clip(jax.random.uniform(splits[6], (BLOCKS, 2, MID), jnp.float32, -2.0, 2.0), -2.0, 2.0),
        "var_mid": jnp.clip(jnp.exp(jax.random.uniform(splits[7], (BLOCKS, 2, MID), jnp.float32, math.log(0.05), math.log(20.0))), 0.05, 20.0),
        "gain_out": jnp.clip(1.0 + 0.1 * jax.random.normal(splits[8], (BLOCKS, CIN), jnp.float32), 0.5, 1.5),
        "bias_out": normal_values(splits[9], (BLOCKS, CIN), 0.5, 3.0, jnp.float32),
        "mean_out": jnp.clip(jax.random.uniform(splits[10], (BLOCKS, CIN), jnp.float32, -2.0, 2.0), -2.0, 2.0),
        "var_out": jnp.clip(jnp.exp(jax.random.uniform(splits[11], (BLOCKS, CIN), jnp.float32, math.log(0.05), math.log(20.0))), 0.05, 20.0),
    }


epsilon = 1e-05
ratio_max = 3.0
shift_max = 5.0

def renorm(z, gain, bias, run_mean, run_var):
    center = lax.optimization_barrier(jnp.mean(z, axis=(0, 1, 2)))
    deviation = z - center
    variance = lax.optimization_barrier(jnp.mean(deviation * deviation, axis=(0, 1, 2)))
    sigma = jnp.sqrt(variance + epsilon)
    run_sigma = jnp.sqrt(run_var + epsilon)
    scale_ratio = jnp.clip(sigma / run_sigma, 1.0 / ratio_max, ratio_max)
    offset_shift = jnp.clip((center - run_mean) / run_sigma, -shift_max, shift_max)
    return gain * (deviation / sigma * scale_ratio + offset_shift) + bias

def reference(images, w_reduce, w_spatial, w_expand, gain_mid, bias_mid, mean_mid, var_mid, gain_out, bias_out, mean_out, var_out):
    current = images
    for block in range(BLOCKS):
        flat = current.reshape(IMAGES * SIDE * SIDE, CIN)
        first = jnp.dot(flat, w_reduce[block], preferred_element_type=jnp.float32).reshape(IMAGES, SIDE, SIDE, MID)
        hidden_one = jax.nn.relu(renorm(first, gain_mid[block, 0], bias_mid[block, 0], mean_mid[block, 0], var_mid[block, 0])).astype(jnp.bfloat16)
        second = lax.conv_general_dilated(hidden_one, w_spatial[block], (1, 1), 'SAME', dimension_numbers=('NHWC', 'HWIO', 'NHWC'), preferred_element_type=jnp.float32)
        hidden_two = jax.nn.relu(renorm(second, gain_mid[block, 1], bias_mid[block, 1], mean_mid[block, 1], var_mid[block, 1])).astype(jnp.bfloat16)
        third = jnp.dot(hidden_two.reshape(IMAGES * SIDE * SIDE, MID), w_expand[block], preferred_element_type=jnp.float32).reshape(IMAGES, SIDE, SIDE, CIN)
        normed = renorm(third, gain_out[block], bias_out[block], mean_out[block], var_out[block])
        current = jax.nn.relu(normed + current.astype(jnp.float32)).astype(jnp.bfloat16)
    return current
```

```python
import functools

import jax
import jax.numpy as jnp
from jax import lax
from jax.experimental import pallas as pl
from jax.experimental.pallas import tpu as pltpu
from jax.sharding import PartitionSpec as P

epsilon = 1e-05
ratio_max = 3.0
shift_max = 5.0
MESH = pl.DeviceIdType.MESH
LANES = 128
f32 = jnp.float32
bf16 = jnp.bfloat16


def coefficients(total, gain, bias, run_mean, run_var, count):
    mean_offset = total[0:1] / count
    center = run_mean + mean_offset
    variance = jnp.maximum(total[1:2] / count - mean_offset * mean_offset, 0.0)
    sigma = jnp.sqrt(variance + epsilon)
    run_sigma = jnp.sqrt(run_var + epsilon)
    ratio = jnp.clip(sigma / run_sigma, 1.0 / ratio_max, ratio_max)
    shift = jnp.clip(mean_offset / run_sigma, -shift_max, shift_max)
    return center, gain * (ratio / sigma), gain * shift + bias


def main_kernel(
    rows,
    cols,
    count,
    side,
    tiles,
    img_ref,
    wr_hbm,
    ws_hbm,
    we_hbm,
    gm_hbm,
    bm_hbm,
    mm_hbm,
    vm_hbm,
    go_hbm,
    bo_hbm,
    mo_hbm,
    vo_hbm,
    x_ref,
    z3_ref,
    coef_ref,
    z_ref,
    hc_ref,
    w2_ref,
    mid_buf,
    out_buf,
    wr_ref,
    we_ref,
    gm_ref,
    bm_ref,
    mm_ref,
    vm_ref,
    go_ref,
    bo_ref,
    mo_ref,
    vo_ref,
    in_sem,
    par_sem,
    tap_sem,
    send_sem,
    recv_sem,
):
    devices = rows * cols
    pixels, images, channels = img_ref.shape
    blocks, _, middle = wr_ref.shape
    slabs = channels // LANES
    line = side * images
    tall = side // tiles
    part = tall * line
    my_row, my_col = lax.axis_index("row"), lax.axis_index("col")
    me = my_row * cols + my_col
    flat_ref = img_ref.reshape(pixels * images, channels)

    def slab_copy(t, c):
        span = pl.ds(t * part, part)
        far = flat_ref.at[span, pl.ds(c * LANES, LANES)]
        return pltpu.make_async_copy(far, x_ref.at[c, span], in_sem.at[t, c])

    pairs = (
        (wr_hbm, wr_ref), (mm_hbm, mm_ref), (we_hbm, we_ref), (gm_hbm, gm_ref),
        (bm_hbm, bm_ref), (vm_hbm, vm_ref), (go_hbm, go_ref), (bo_hbm, bo_ref),
        (mo_hbm, mo_ref), (vo_hbm, vo_ref),
    )
    loads = [pltpu.make_async_copy(a, b, par_sem.at[i]) for i, (a, b) in enumerate(pairs)]
    kernels = [
        pltpu.make_async_copy(
            ws_hbm.at[block],
            w2_ref.at[block, pl.ds(3 * i * middle, 9 * middle), pl.ds(i * middle, middle)],
            tap_sem.at[block, i],
        )
        for block in range(blocks)
        for i in range(2)
    ]
    for copy in loads[:2]:
        copy.start()
    for t in range(tiles):
        for c in range(slabs):
            slab_copy(t, c).start()
    for copy in loads[2:] + kernels:
        copy.start()

    barrier = pltpu.get_barrier_semaphore()

    def to_all(act):
        if devices <= 64:
            far_rows = [lax.rem(my_row + i, rows) for i in range(rows)]
            far_cols = [lax.rem(my_col + i, cols) for i in range(cols)]
            for j in range(cols - 1, -1, -1):
                for i in range(rows):
                    if i or j:
                        act((far_rows[i], far_cols[j]))
        else:

            def step(i, c):
                other = lax.rem(me + i, devices)
                act((lax.div(other, cols), lax.rem(other, cols)))
                return c

            lax.fori_loop(1, devices, step, 0)

    to_all(
        lambda there: pl.semaphore_signal(
            barrier, inc=1, device_id=there, device_id_type=MESH
        )
    )

    def exchange(buf, slot, sums, gain, bias, mean, var, index, first):
        for i in range(2):
            buf[slot, me, pl.ds(i, 1), :] = jnp.sum(sums[i], axis=0, keepdims=True)
        if first:
            pl.semaphore_wait(barrier, devices - 1)

        def send(there):
            pltpu.make_async_remote_copy(
                src_ref=buf.at[slot, me],
                dst_ref=buf.at[slot, me],
                send_sem=send_sem.at[index],
                recv_sem=recv_sem.at[index],
                device_id=there,
                device_id_type=MESH,
            ).start()

        to_all(send)
        others = buf.at[slot, pl.ds(0, devices - 1)]
        whole = pltpu.make_async_remote_copy(
            src_ref=others,
            dst_ref=others,
            send_sem=send_sem.at[index],
            recv_sem=recv_sem.at[index],
            device_id=(lax.rem(my_row + 1, rows), my_col),
            device_id_type=MESH,
        )
        whole.wait_send()
        whole.wait_recv()
        total = jnp.sum(buf[slot], axis=0)
        return coefficients(total, gain, bias, mean, var, count)

    def moments(z, mean, sums):
        d = (z - mean).reshape(-1, 16, z.shape[-1])
        return sums[0] + jnp.sum(d, axis=0), sums[1] + jnp.sum(d * d, axis=0)

    def zeros(c):
        return (jnp.zeros((16, c), f32), jnp.zeros((16, c), f32))

    hc_ref[0] = jnp.zeros((line, 3 * middle), bf16)
    hc_ref[side + 1] = jnp.zeros((line, 3 * middle), bf16)
    empty = jnp.zeros((3 * middle, middle), bf16)
    for block in range(blocks):
        w2_ref[block, pl.ds(9 * middle, 3 * middle), 0:middle] = empty
        w2_ref[block, pl.ds(0, 3 * middle), middle : 2 * middle] = empty
    for copy in loads[:2]:
        copy.wait()
    place = lax.broadcasted_iota(jnp.int32, (1, line, 1), 1)

    def updated(t, coef):
        center, scale, offset = coef
        span = pl.ds(pl.multiple_of(t * part, 16), part)
        new = []
        for c in range(slabs):
            lanes = slice(c * LANES, (c + 1) * LANES)
            z = (z3_ref[span, lanes] - center[:, lanes]) * scale[:, lanes] + offset[:, lanes]
            y = jnp.maximum(z + x_ref[c, span, :].astype(f32), 0.0).astype(bf16)
            x_ref[c, span, :] = y
            new.append(y)
        return new

    out_coef = None
    for block in range(blocks):
        mean_one = mm_ref[block, pl.ds(0, 1), :]
        mean_two = mm_ref[block, pl.ds(1, 1), :]

        def reduce_step(t, sums):
            if block == 0:
                for c in range(slabs):
                    slab_copy(t, c).wait()
                span = pl.ds(pl.multiple_of(t * part, 16), part)
                x = [x_ref[c, span, :] for c in range(slabs)]
            else:
                x = updated(t, out_coef)
            x = jnp.concatenate(x, axis=1)
            z = jnp.dot(x, wr_ref[block], preferred_element_type=f32)
            z_ref[t] = z.reshape(tall // 2, 2, line, middle)
            return moments(z, mean_one, sums)

        sums = lax.fori_loop(0, tiles, reduce_step, zeros(middle), unroll=True)
        if block == 0:
            for copy in loads[2:] + kernels:
                copy.wait()
        mean_out = mo_ref[pl.ds(block, 1), :]
        center1, scale1, offset1 = exchange(
            mid_buf, 2 * block, sums,
            gm_ref[block, pl.ds(0, 1), :], bm_ref[block, pl.ds(0, 1), :],
            mean_one, vm_ref[block, pl.ds(0, 1), :], 3 * block, block == 0,
        )

        def taps_step(t, carry):
            z = z_ref[t].reshape(part, middle)
            h = jnp.maximum((z - center1) * scale1 + offset1, 0.0)
            left = pltpu.roll(h, images, 0).reshape(tall, line, middle)
            right = pltpu.roll(h, part - images, 0).reshape(tall, line, middle)
            left = jnp.where(place >= images, left, 0.0)
            right = jnp.where(place < line - images, right, 0.0)
            taps = (left, h.reshape(tall, line, middle), right)
            for i, tap in enumerate(taps):
                lanes = slice(i * middle, (i + 1) * middle)
                hc_ref[pl.ds(t * tall + 1, tall), :, lanes] = tap.astype(bf16)
            return carry

        def conv_step(t, sums):
            v = hc_ref[pl.ds(t * tall, tall + 2)].reshape(tall // 2 + 1, 2, line, 3 * middle)
            lhs = jnp.concatenate(
                [v[:-1, 0], v[:-1, 1], v[1:, 0], v[1:, 1]], axis=-1
            ).reshape(part // 2, 12 * middle)
            z = jnp.dot(lhs, w2_ref[block], preferred_element_type=f32)
            for i in range(2):
                half = z[:, i * middle : (i + 1) * middle]
                z_ref[t, :, i] = half.reshape(tall // 2, line, middle)
                sums = moments(half, mean_two, sums)
            return sums

        lax.fori_loop(0, tiles, taps_step, 0, unroll=True)
        sums = lax.fori_loop(0, tiles, conv_step, zeros(middle), unroll=True)
        center2, scale2, offset2 = exchange(
            mid_buf, 2 * block + 1, sums,
            gm_ref[block, pl.ds(1, 1), :], bm_ref[block, pl.ds(1, 1), :],
            mean_two, vm_ref[block, pl.ds(1, 1), :], 3 * block + 1, False,
        )

        def expand_step(t, sums):
            z = z_ref[t].reshape(part, middle)
            h = jnp.maximum((z - center2) * scale2 + offset2, 0.0).astype(bf16)
            z = jnp.dot(h, we_ref[block], preferred_element_type=f32)
            z3_ref[pl.ds(pl.multiple_of(t * part, 16), part), :] = z
            return moments(z, mean_out, sums)

        sums = lax.fori_loop(0, tiles, expand_step, zeros(channels), unroll=True)
        out_coef = exchange(
            out_buf, block, sums,
            go_ref[pl.ds(block, 1), :], bo_ref[pl.ds(block, 1), :],
            mean_out, vo_ref[pl.ds(block, 1), :], 3 * block + 2, False,
        )

    for i in range(3):
        coef_ref[pl.ds(i, 1), :] = out_coef[i]


def last_kernel(pieces, x_ref, z3_ref, coef_ref, o_ref, y_ref, out_sem):
    slabs = x_ref.shape[0]
    pixels, images, channels = o_ref.shape
    part = pixels // pieces * images
    flat_ref = o_ref.reshape(pixels * images, channels)

    def slab_copy(t, c):
        span = pl.ds(t * part, part)
        far = flat_ref.at[span, pl.ds(c * LANES, LANES)]
        return pltpu.make_async_copy(y_ref.at[c, span], far, out_sem.at[t, c])

    def step(t, carry):
        span = pl.ds(pl.multiple_of(t * part, 16), part)
        for c in range(slabs):
            lanes = slice(c * LANES, (c + 1) * LANES)
            center, scale, offset = (coef_ref[pl.ds(i, 1), lanes] for i in range(3))
            z = (z3_ref[span, lanes] - center) * scale + offset
            y = jnp.maximum(z + x_ref[c, span, :].astype(f32), 0.0)
            y_ref[c, span, :] = y.astype(bf16)
            slab_copy(t, c).start()
        return carry

    lax.fori_loop(0, pieces, step, 0)
    for t in range(pieces):
        for c in range(slabs):
            slab_copy(t, c).wait()


def local(mesh_rows, mesh_cols, images, w_reduce, w_spatial, w_expand, *params):
    held, side, _, channels = images.shape
    blocks, _, middle = w_reduce.shape
    devices = mesh_rows * mesh_cols
    count = float(held * side * side * devices)
    tiles = next(t for t in (TILES, 2, 1) if side % (2 * t) == 0)
    slabs = channels // LANES
    pixels = side * side
    vmem = pl.BlockSpec(memory_space=pltpu.VMEM)
    anywhere = pl.BlockSpec(memory_space=pltpu.HBM)
    turned = images.transpose(1, 2, 0, 3).reshape(pixels, held, channels)
    taps = w_spatial.reshape(blocks, 9 * middle, middle)
    operands = [
        pltpu.with_memory_space_constraint(a, pltpu.HBM)
        for a in (turned, w_reduce, taps, w_expand, *params)
    ]
    x, z3, coef = pl.pallas_call(
        functools.partial(main_kernel, mesh_rows, mesh_cols, count, side, tiles),
        out_shape=(
            jax.ShapeDtypeStruct((slabs, pixels * held, LANES), bf16),
            jax.ShapeDtypeStruct((pixels * held, channels), f32),
            jax.ShapeDtypeStruct((3, channels), f32),
        ),
        in_specs=[anywhere] * 12,
        out_specs=(vmem, vmem, vmem),
        scratch_shapes=[
            pltpu.VMEM((tiles, side // tiles // 2, 2, side * held, middle), f32),
            pltpu.VMEM((side + 2, side * held, 3 * middle), bf16),
            pltpu.VMEM((blocks, 12 * middle, 2 * middle), bf16),
            pltpu.VMEM((2 * blocks, devices, 2, middle), f32),
            pltpu.VMEM((blocks, devices, 2, channels), f32),
            pltpu.VMEM(w_reduce.shape, bf16),
            pltpu.VMEM(w_expand.shape, bf16),
            *(pltpu.VMEM(p.shape, f32) for p in params),
            pltpu.SemaphoreType.DMA((tiles, slabs)),
            pltpu.SemaphoreType.DMA((10,)),
            pltpu.SemaphoreType.DMA((blocks, 2)),
            pltpu.SemaphoreType.DMA((3 * blocks,)),
            pltpu.SemaphoreType.DMA((3 * blocks,)),
        ],
        compiler_params=pltpu.CompilerParams(
            collective_id=0, has_side_effects=True, vmem_limit_bytes=LIMIT * 1024 * 1024
        ),
        name="bottlenecks",
    )(*operands)
    pieces = side // 4 if side % 4 == 0 else 1
    out = pl.pallas_call(
        functools.partial(last_kernel, pieces),
        out_shape=jax.ShapeDtypeStruct((pixels, held, channels), bf16),
        in_specs=[vmem] * 3,
        out_specs=anywhere,
        scratch_shapes=[
            pltpu.VMEM((slabs, pixels * held, LANES), bf16),
            pltpu.SemaphoreType.DMA((pieces, slabs)),
        ],
        compiler_params=pltpu.CompilerParams(vmem_limit_bytes=16 * 1024 * 1024),
        name="finish",
    )(x, z3, coef)
    return out.reshape(side, side, held, channels).transpose(2, 0, 1, 3)


TILES = 2
LIMIT = 32


def solution(mesh):
    spec = P(("row", "col"), None, None, None)
    return jax.shard_map(
        functools.partial(local, mesh.shape["row"], mesh.shape["col"]),
        mesh=mesh,
        in_specs=(spec,) + (P(),) * 11,
        out_specs=spec,
        check_vma=False,
    )
```

```python
import functools

import jax
import jax.numpy as jnp
from jax import lax
from jax.experimental import pallas as pl
from jax.experimental.pallas import tpu as pltpu
from jax.sharding import PartitionSpec as P

epsilon = 1e-05
ratio_max = 3.0
shift_max = 5.0
MESH = pl.DeviceIdType.MESH
LANES = 128
f32 = jnp.float32
bf16 = jnp.bfloat16


def coefficients(total, gain, bias, run_mean, run_var, count):
    mean_offset = total[0:1] / count
    center = run_mean + mean_offset
    variance = jnp.maximum(total[1:2] / count - mean_offset * mean_offset, 0.0)
    sigma = jnp.sqrt(variance + epsilon)
    run_sigma = jnp.sqrt(run_var + epsilon)
    ratio = jnp.clip(sigma / run_sigma, 1.0 / ratio_max, ratio_max)
    shift = jnp.clip(mean_offset / run_sigma, -shift_max, shift_max)
    scale = gain * (ratio / sigma)
    return scale, gain * shift + bias - center * scale


def flipped(index, bits):
    out, bit = index, 1
    while bit <= bits:
        if bits & bit:
            out = out + bit - 2 * bit * lax.rem(lax.div(index, bit), 2)
        bit *= 2
    return out


def tree_sum(parts):
    while len(parts) > 1:
        half = [a + b for a, b in zip(parts[0::2], parts[1::2])]
        parts = half + ([parts[-1]] if len(parts) % 2 else [])
    return parts[0]


def group_width(channels):
    return 2 * LANES if channels % (2 * LANES) == 0 else channels


def main_kernel(
    rows,
    cols,
    count,
    side,
    tiles,
    loads_in,
    img_ref,
    wr_hbm,
    ws_hbm,
    we_hbm,
    gm_hbm,
    bm_hbm,
    mm_hbm,
    vm_hbm,
    go_hbm,
    bo_hbm,
    mo_hbm,
    vo_hbm,
    x_ref,
    z3_ref,
    coef_ref,
    z_ref,
    h_ref,
    hc_ref,
    w2_ref,
    mid_buf,
    out_buf,
    wr_ref,
    we_ref,
    gm_ref,
    bm_ref,
    mm_ref,
    vm_ref,
    go_ref,
    bo_ref,
    mo_ref,
    vo_ref,
    in_sem,
    par_sem,
    tap_sem,
    send_sem,
    recv_sem,
):
    devices = rows * cols
    pixels, images, channels = img_ref.shape
    blocks, _, middle = wr_ref.shape
    slabs = channels // LANES
    width = group_width(channels)
    groups = channels // width
    per = width // LANES
    line = side * images
    tall = side // tiles
    part = tall * line
    total_rows = pixels * images
    my_row, my_col = lax.axis_index("row"), lax.axis_index("col")
    me = my_row * cols + my_col
    flat_ref = img_ref.reshape(total_rows, channels)
    zf_ref = z_ref.reshape(total_rows, middle)
    piece = total_rows // loads_in

    def slab_copy(t, c):
        span = pl.ds(t * piece, piece)
        far = flat_ref.at[span, pl.ds(c * LANES, LANES)]
        return pltpu.make_async_copy(far, x_ref.at[c, span], in_sem.at[t, c])

    pairs = (
        (wr_hbm, wr_ref), (mm_hbm, mm_ref), (we_hbm, we_ref), (gm_hbm, gm_ref),
        (bm_hbm, bm_ref), (vm_hbm, vm_ref), (go_hbm, go_ref), (bo_hbm, bo_ref),
        (mo_hbm, mo_ref), (vo_hbm, vo_ref),
    )
    loads = [pltpu.make_async_copy(a, b, par_sem.at[i]) for i, (a, b) in enumerate(pairs)]
    kernels = [
        pltpu.make_async_copy(
            ws_hbm.at[block],
            w2_ref.at[block, pl.ds(3 * i * middle, 9 * middle), pl.ds(i * middle, middle)],
            tap_sem.at[block, i],
        )
        for block in range(blocks)
        for i in range(2)
    ]
    for copy in loads[:2]:
        copy.start()
    for t in range(loads_in):
        for c in range(slabs):
            slab_copy(t, c).start()

    barrier = pltpu.get_barrier_semaphore()

    def to_all(act):
        if devices <= 64:
            if rows & (rows - 1) == 0 and cols & (cols - 1) == 0:
                far_rows = [flipped(my_row, i) for i in range(rows)]
                far_cols = [flipped(my_col, i) for i in range(cols)]
            else:
                far_rows = [lax.rem(my_row + i, rows) for i in range(rows)]
                far_cols = [lax.rem(my_col + i, cols) for i in range(cols)]
            for j in range(cols - 1, -1, -1):
                for i in range(rows - 1, -1, -1):
                    if i or j:
                        act((far_rows[i], far_cols[j]))
        else:

            def step(i, c):
                other = lax.rem(me + i, devices)
                act((lax.div(other, cols), lax.rem(other, cols)))
                return c

            lax.fori_loop(1, devices, step, 0)

    to_all(
        lambda there: pl.semaphore_signal(
            barrier, inc=1, device_id=there, device_id_type=MESH
        )
    )

    def slots(ref, index):
        others = ref.at[pl.ds(0, devices - 1)]
        return pltpu.make_async_remote_copy(
            src_ref=others,
            dst_ref=others,
            send_sem=send_sem.at[index],
            recv_sem=recv_sem.at[index],
            device_id=(lax.rem(my_row + 1, rows), my_col),
            device_id_type=MESH,
        )

    def share(ref, sums, index):
        for i in range(2):
            ref[me, pl.ds(i, 1), :] = jnp.sum(sums[i], axis=0, keepdims=True)
        if index == 0:
            pl.semaphore_wait(barrier, devices - 1)

        def send(there):
            pltpu.make_async_remote_copy(
                src_ref=ref.at[me],
                dst_ref=ref.at[me],
                send_sem=send_sem.at[index],
                recv_sem=recv_sem.at[index],
                device_id=there,
                device_id_type=MESH,
            ).start()

        to_all(send)

    def collect(ref, index):
        slots(ref, index).wait_recv()
        if devices <= 64:
            return tree_sum([ref[d] for d in range(devices)])
        return jnp.sum(ref[...], axis=0)

    def moments(z, mean, sums):
        d = (z - mean).reshape(-1, 16, z.shape[-1])
        return sums[0] + jnp.sum(d, axis=0), sums[1] + jnp.sum(d * d, axis=0)

    def zeros(c):
        return (jnp.zeros((16, c), f32), jnp.zeros((16, c), f32))

    hc_ref[0] = jnp.zeros((line, 3 * middle), bf16)
    hc_ref[side + 1] = jnp.zeros((line, 3 * middle), bf16)
    empty = jnp.zeros((3 * middle, middle), bf16)
    for block in range(blocks):
        w2_ref[block, pl.ds(9 * middle, 3 * middle), 0:middle] = empty
        w2_ref[block, pl.ds(0, 3 * middle), middle : 2 * middle] = empty
    for copy in loads[:2]:
        copy.wait()
    place = lax.broadcasted_iota(jnp.int32, (1, line, 1), 1)

    def updated(start, size, g, coef):
        scale, offset = coef
        new = []
        for c in range(per):
            lanes = slice(c * LANES, (c + 1) * LANES)
            slab = g * per + c
            span = pl.ds(start, size)
            z = z3_ref[slab, span, :] * scale[:, lanes] + offset[:, lanes]
            y = jnp.maximum(z + x_ref[slab, span, :].astype(f32), 0.0).astype(bf16)
            x_ref[slab, span, :] = y
            new.append(y)
        return new

    def halves(start, size):
        first = (size // 2 + 15) // 16 * 16
        return ((start, first), (start + first, size - first))

    per_block = 2 + groups

    def index_of(block, stage):
        return per_block * block + stage

    mids = lambda block, i: mid_buf.at[2 * block + i]
    outs = lambda block, g: out_buf.at[block, g]

    sums = zeros(middle)
    mean_one = mm_ref[0, pl.ds(0, 1), :]
    for t in range(loads_in):
        for c in range(slabs):
            slab_copy(t, c).wait()
        for start, size in halves(t * piece, piece):
            x = jnp.concatenate([x_ref[c, pl.ds(start, size), :] for c in range(slabs)], axis=1)
            z = jnp.dot(x, wr_ref[0], preferred_element_type=f32)
            zf_ref[pl.ds(start, size), :] = z
            sums = moments(z, mean_one, sums)
    share(mids(0, 0), sums, index_of(0, 0))
    for copy in loads[2:] + kernels:
        copy.start()
    for copy in loads[2:] + kernels:
        copy.wait()

    for block in range(blocks):
        mean_one = mm_ref[block, pl.ds(0, 1), :]
        mean_two = mm_ref[block, pl.ds(1, 1), :]
        scale1, offset1 = coefficients(
            collect(mids(block, 0), index_of(block, 0)),
            gm_ref[block, pl.ds(0, 1), :], bm_ref[block, pl.ds(0, 1), :],
            mean_one, vm_ref[block, pl.ds(0, 1), :], count,
        )

        for t in range(tiles):
            z = zf_ref[pl.ds(t * part, part), :]
            h = jnp.maximum(z * scale1 + offset1, 0.0)
            left = pltpu.roll(h, images, 0).reshape(tall, line, middle)
            right = pltpu.roll(h, part - images, 0).reshape(tall, line, middle)
            left = jnp.where(place >= images, left, 0.0)
            right = jnp.where(place < line - images, right, 0.0)
            taps = (left, h.reshape(tall, line, middle), right)
            for i, tap in enumerate(taps):
                lanes = slice(i * middle, (i + 1) * middle)
                hc_ref[pl.ds(t * tall + 1, tall), :, lanes] = tap.astype(bf16)

        sums = zeros(middle)
        for t in range(tiles):
            v = hc_ref[pl.ds(t * tall, tall + 2)].reshape(tall // 2 + 1, 2, line, 3 * middle)
            lhs = jnp.concatenate(
                [v[:-1, 0], v[:-1, 1], v[1:, 0], v[1:, 1]], axis=-1
            ).reshape(part // 2, 12 * middle)
            z = jnp.dot(lhs, w2_ref[block], preferred_element_type=f32)
            for i in range(2):
                half = z[:, i * middle : (i + 1) * middle]
                z_ref[pl.ds(t * (tall // 2), tall // 2), i] = half.reshape(
                    tall // 2, line, middle
                )
                sums = moments(half, mean_two, sums)
        share(mids(block, 1), sums, index_of(block, 1))
        scale2, offset2 = coefficients(
            collect(mids(block, 1), index_of(block, 1)),
            gm_ref[block, pl.ds(1, 1), :], bm_ref[block, pl.ds(1, 1), :],
            mean_two, vm_ref[block, pl.ds(1, 1), :], count,
        )

        for g in range(groups):
            wide = slice(g * width, (g + 1) * width)
            mean_out = mo_ref[pl.ds(block, 1), wide]
            sums = zeros(width)
            for t in range(tiles):
                span = pl.ds(t * part, part)
                if g == 0:
                    z = zf_ref[span, :]
                    h = jnp.maximum(z * scale2 + offset2, 0.0).astype(bf16)
                    h_ref[span, :] = h
                else:
                    h = h_ref[span, :]
                z = jnp.dot(h, we_ref[block, :, wide], preferred_element_type=f32)
                for c in range(per):
                    z3_ref[g * per + c, span, :] = z[:, c * LANES : (c + 1) * LANES]
                sums = moments(z, mean_out, sums)
            share(outs(block, g), sums, index_of(block, 2 + g))

        last = block == blocks - 1
        if not last:
            mean_one = mm_ref[block + 1, pl.ds(0, 1), :]
            sums = zeros(middle)
        for g in range(groups):
            wide = slice(g * width, (g + 1) * width)
            coef = coefficients(
                collect(outs(block, g), index_of(block, 2 + g)),
                go_ref[pl.ds(block, 1), wide], bo_ref[pl.ds(block, 1), wide],
                mo_ref[pl.ds(block, 1), wide], vo_ref[pl.ds(block, 1), wide], count,
            )
            if last and g == groups - 1:
                for i in range(2):
                    coef_ref[pl.ds(i, 1), :] = coef[i]
                break
            for t in range(tiles):
                y = updated(t * part, part, g, coef)
                if last:
                    continue
                span = pl.ds(t * part, part)
                y = jnp.concatenate(y, axis=1)
                z = jnp.dot(y, wr_ref[block + 1, wide, :], preferred_element_type=f32)
                if g:
                    z = z + zf_ref[span, :]
                zf_ref[span, :] = z
                if g == groups - 1:
                    sums = moments(z, mean_one, sums)
        if not last:
            share(mids(block + 1, 0), sums, index_of(block + 1, 0))

    for block in range(blocks):
        for i in range(2):
            slots(mids(block, i), index_of(block, i)).wait_send()
        for g in range(groups):
            slots(outs(block, g), index_of(block, 2 + g)).wait_send()


def last_kernel(pieces, x_ref, z3_ref, coef_ref, o_ref, y_ref, out_sem, old_sem):
    slabs = x_ref.shape[0]
    pixels, images, channels = o_ref.shape
    part = pixels // pieces * images
    per = coef_ref.shape[1] // LANES
    done = slabs - per
    flat_ref = o_ref.reshape(pixels * images, channels)

    def old_copy(c):
        return pltpu.make_async_copy(
            x_ref.at[c], flat_ref.at[:, pl.ds(c * LANES, LANES)], old_sem.at[c]
        )

    def slab_copy(t, c):
        span = pl.ds(t * part, part)
        far = flat_ref.at[span, pl.ds((done + c) * LANES, LANES)]
        return pltpu.make_async_copy(y_ref.at[c, span], far, out_sem.at[t, c])

    for c in range(done):
        old_copy(c).start()

    def step(t, carry):
        span = pl.ds(pl.multiple_of(t * part, 16), part)
        for c in range(per):
            lanes = slice(c * LANES, (c + 1) * LANES)
            scale, offset = (coef_ref[pl.ds(i, 1), lanes] for i in range(2))
            z = z3_ref[done + c, span, :] * scale + offset
            y = jnp.maximum(z + x_ref[done + c, span, :].astype(f32), 0.0)
            y_ref[c, span, :] = y.astype(bf16)
            slab_copy(t, c).start()
        return carry

    lax.fori_loop(0, pieces, step, 0)
    for c in range(done):
        old_copy(c).wait()
    for t in range(pieces):
        for c in range(per):
            slab_copy(t, c).wait()


def local(mesh_rows, mesh_cols, images, w_reduce, w_spatial, w_expand, *params):
    held, side, _, channels = images.shape
    blocks, _, middle = w_reduce.shape
    devices = mesh_rows * mesh_cols
    count = float(held * side * side * devices)
    tiles = next(t for t in (TILES, 2, 1) if side % (2 * t) == 0)
    slabs = channels // LANES
    pixels = side * side
    loads_in = next(t for t in (4, 2, 1) if pixels * held % (16 * t) == 0)
    width = group_width(channels)
    groups = channels // width
    vmem = pl.BlockSpec(memory_space=pltpu.VMEM)
    anywhere = pl.BlockSpec(memory_space=pltpu.HBM)
    turned = images.transpose(1, 2, 0, 3).reshape(pixels, held, channels)
    taps = w_spatial.reshape(blocks, 9 * middle, middle)
    operands = [
        pltpu.with_memory_space_constraint(a, pltpu.HBM)
        for a in (turned, w_reduce, taps, w_expand, *params)
    ]
    x, z3, coef = pl.pallas_call(
        functools.partial(main_kernel, mesh_rows, mesh_cols, count, side, tiles, loads_in),
        out_shape=(
            jax.ShapeDtypeStruct((slabs, pixels * held, LANES), bf16),
            jax.ShapeDtypeStruct((slabs, pixels * held, LANES), f32),
            jax.ShapeDtypeStruct((2, width), f32),
        ),
        in_specs=[anywhere] * 12,
        out_specs=(vmem, vmem, vmem),
        scratch_shapes=[
            pltpu.VMEM((side // 2, 2, side * held, middle), f32),
            pltpu.VMEM((pixels * held, middle), bf16),
            pltpu.VMEM((side + 2, side * held, 3 * middle), bf16),
            pltpu.VMEM((blocks, 12 * middle, 2 * middle), bf16),
            pltpu.VMEM((2 * blocks, devices, 2, middle), f32),
            pltpu.VMEM((blocks, groups, devices, 2, width), f32),
            pltpu.VMEM(w_reduce.shape, bf16),
            pltpu.VMEM(w_expand.shape, bf16),
            *(pltpu.VMEM(p.shape, f32) for p in params),
            pltpu.SemaphoreType.DMA((loads_in, slabs)),
            pltpu.SemaphoreType.DMA((10,)),
            pltpu.SemaphoreType.DMA((blocks, 2)),
            pltpu.SemaphoreType.DMA(((2 + groups) * blocks,)),
            pltpu.SemaphoreType.DMA(((2 + groups) * blocks,)),
        ],
        compiler_params=pltpu.CompilerParams(
            collective_id=0, has_side_effects=True, vmem_limit_bytes=LIMIT * 1024 * 1024
        ),
        name="bottlenecks",
    )(*operands)
    pieces = side // 4 if side % 4 == 0 else 1
    out = pl.pallas_call(
        functools.partial(last_kernel, pieces),
        out_shape=jax.ShapeDtypeStruct((pixels, held, channels), bf16),
        in_specs=[vmem] * 3,
        out_specs=anywhere,
        scratch_shapes=[
            pltpu.VMEM((width // LANES, pixels * held, LANES), bf16),
            pltpu.SemaphoreType.DMA((pieces, width // LANES)),
            pltpu.SemaphoreType.DMA((slabs,)),
        ],
        compiler_params=pltpu.CompilerParams(vmem_limit_bytes=16 * 1024 * 1024),
        name="finish",
    )(x, z3, coef)
    return out.reshape(side, side, held, channels).transpose(2, 0, 1, 3)


TILES = 2
LIMIT = 32


def solution(mesh):
    spec = P(("row", "col"), None, None, None)
    return jax.shard_map(
        functools.partial(local, mesh.shape["row"], mesh.shape["col"]),
        mesh=mesh,
        in_specs=(spec,) + (P(),) * 11,
        out_specs=spec,
        check_vma=False,
    )
```

```python
import functools

import jax
import jax.numpy as jnp
from jax import lax
from jax.experimental import pallas as pl
from jax.experimental.pallas import tpu as pltpu
from jax.sharding import PartitionSpec as P

epsilon = 1e-05
ratio_max = 3.0
shift_max = 5.0
MESH = pl.DeviceIdType.MESH
LANES = 128
f32 = jnp.float32
bf16 = jnp.bfloat16


def coefficients(total, gain, bias, run_var, count):
    mean_offset = total[0:1] / count
    variance = jnp.maximum(total[1:2] / count - mean_offset * mean_offset, 0.0)
    sigma = jnp.sqrt(variance + epsilon)
    run_sigma = jnp.sqrt(run_var + epsilon)
    ratio = jnp.clip(sigma / run_sigma, 1.0 / ratio_max, ratio_max)
    shift = jnp.clip(mean_offset / run_sigma, -shift_max, shift_max)
    scale = gain * (ratio / sigma)
    return scale, gain * shift + bias - mean_offset * scale


def flipped(index, bits):
    out, bit = index, 1
    while bit <= bits:
        if bits & bit:
            out = out + bit - 2 * bit * lax.rem(lax.div(index, bit), 2)
        bit *= 2
    return out


def tree_sum(parts):
    while len(parts) > 1:
        half = [a + b for a, b in zip(parts[0::2], parts[1::2])]
        parts = half + ([parts[-1]] if len(parts) % 2 else [])
    return parts[0]


def group_width(channels):
    return 2 * LANES if channels % (2 * LANES) == 0 else channels


def main_kernel(
    rows,
    cols,
    count,
    side,
    tiles,
    loads_in,
    img_ref,
    wr_hbm,
    ws_hbm,
    we_hbm,
    gm_hbm,
    bm_hbm,
    mm_hbm,
    vm_hbm,
    go_hbm,
    bo_hbm,
    mo_hbm,
    vo_hbm,
    x_ref,
    z3_ref,
    coef_ref,
    z_ref,
    h_ref,
    hc_ref,
    w2_ref,
    mid_buf,
    out_buf,
    wr_ref,
    we_ref,
    gm_ref,
    bm_ref,
    mm_ref,
    vm_ref,
    go_ref,
    bo_ref,
    mo_ref,
    vo_ref,
    in_sem,
    par_sem,
    tap_sem,
    send_sem,
    recv_sem,
):
    devices = rows * cols
    pixels, images, channels = img_ref.shape
    blocks, _, middle = wr_ref.shape
    slabs = channels // LANES
    width = group_width(channels)
    groups = channels // width
    per = width // LANES
    line = side * images
    tall = side // tiles
    part = tall * line
    total_rows = pixels * images
    my_row, my_col = lax.axis_index("row"), lax.axis_index("col")
    me = my_row * cols + my_col
    flat_ref = img_ref.reshape(total_rows, channels)
    zf_ref = z_ref.reshape(total_rows, middle)
    piece = total_rows // loads_in

    def slab_copy(t, c):
        span = pl.ds(t * piece, piece)
        far = flat_ref.at[span, pl.ds(c * LANES, LANES)]
        return pltpu.make_async_copy(far, x_ref.at[c, span], in_sem.at[t, c])

    pairs = (
        (wr_hbm.at[0], wr_ref.at[0]), (mm_hbm, mm_ref), (we_hbm, we_ref.at[:, pl.ds(0, middle)]), (gm_hbm, gm_ref),
        (bm_hbm, bm_ref), (vm_hbm, vm_ref), (go_hbm, go_ref), (bo_hbm, bo_ref),
        (mo_hbm, mo_ref), (vo_hbm, vo_ref),
    )
    loads = [pltpu.make_async_copy(a, b, par_sem.at[i]) for i, (a, b) in enumerate(pairs)]
    if blocks > 1:
        rest = pl.ds(1, blocks - 1)
        loads.append(pltpu.make_async_copy(wr_hbm.at[rest], wr_ref.at[rest], par_sem.at[len(pairs)]))
    kernels = [
        pltpu.make_async_copy(
            ws_hbm.at[block],
            w2_ref.at[block, pl.ds(3 * i * middle, 9 * middle), pl.ds(i * middle, middle)],
            tap_sem.at[block, i],
        )
        for block in range(blocks)
        for i in range(2)
    ]
    barrier = pltpu.get_barrier_semaphore()

    def to_all(act):
        if devices <= 64:
            if rows & (rows - 1) == 0 and cols & (cols - 1) == 0:
                far_rows = [flipped(my_row, i) for i in range(rows)]
                far_cols = [flipped(my_col, i) for i in range(cols)]
            else:
                far_rows = [lax.rem(my_row + i, rows) for i in range(rows)]
                far_cols = [lax.rem(my_col + i, cols) for i in range(cols)]
            for j in range(cols - 1, -1, -1):
                for i in range(rows - 1, -1, -1):
                    if i or j:
                        act((far_rows[i], far_cols[j]))
        else:

            def step(i, c):
                other = lax.rem(me + i, devices)
                act((lax.div(other, cols), lax.rem(other, cols)))
                return c

            lax.fori_loop(1, devices, step, 0)

    for copy in loads[:2]:
        copy.start()
    to_all(
        lambda there: pl.semaphore_signal(
            barrier, inc=1, device_id=there, device_id_type=MESH
        )
    )

    for t in range(loads_in):
        for c in range(slabs):
            slab_copy(t, c).start()

    def slots(ref, index):
        others = ref.at[pl.ds(0, devices - 1)]
        return pltpu.make_async_remote_copy(
            src_ref=others,
            dst_ref=others,
            send_sem=send_sem.at[index],
            recv_sem=recv_sem.at[index],
            device_id=(lax.rem(my_row + 1, rows), my_col),
            device_id_type=MESH,
        )

    def share(ref, sums, index):
        for i in range(2):
            ref[me, pl.ds(i, 1), :] = jnp.sum(sums[i], axis=0, keepdims=True)
        if index == 0:
            pl.semaphore_wait(barrier, devices - 1)

        def send(there):
            pltpu.make_async_remote_copy(
                src_ref=ref.at[me],
                dst_ref=ref.at[me],
                send_sem=send_sem.at[index],
                recv_sem=recv_sem.at[index],
                device_id=there,
                device_id_type=MESH,
            ).start()

        to_all(send)

    def collect(ref, index):
        slots(ref, index).wait_recv()
        if devices <= 64:
            return tree_sum([ref[d] for d in range(devices)])
        return jnp.sum(ref[...], axis=0)

    def moments(d, sums):
        d = d.reshape(-1, 16, d.shape[-1])
        return sums[0] + jnp.sum(d, axis=0), sums[1] + jnp.sum(d * d, axis=0)

    def zeros(c):
        return (jnp.zeros((16, c), f32), jnp.zeros((16, c), f32))

    for copy in loads[:2]:
        copy.wait()
    place = lax.broadcasted_iota(jnp.int32, (1, line, 1), 1)

    def updated(start, size, g, coef):
        scale, offset = coef
        new = []
        for c in range(per):
            lanes = slice(c * LANES, (c + 1) * LANES)
            slab = g * per + c
            span = pl.ds(start, size)
            z = z3_ref[slab, span, :] * scale[:, lanes] + offset[:, lanes]
            y = jnp.maximum(z.astype(bf16) + x_ref[slab, span, :], 0)
            x_ref[slab, span, :] = y
            new.append(y)
        return new

    def halves(start, size):
        first = (size // 2 + 15) // 16 * 16
        return ((start, first), (start + first, size - first))

    per_block = 2 + groups

    def index_of(block, stage):
        return per_block * block + stage

    mids = lambda block, i: mid_buf.at[2 * block + i]
    outs = lambda block, g: out_buf.at[block, g]

    sums = zeros(middle)
    mean_one = mm_ref[0, pl.ds(0, 1), :]
    for t in range(loads_in):
        for c in range(slabs):
            slab_copy(t, c).wait()
        for start, size in halves(t * piece, piece):
            x = jnp.concatenate([x_ref[c, pl.ds(start, size), :] for c in range(slabs)], axis=1)
            z = jnp.dot(x, wr_ref[0], preferred_element_type=f32) - mean_one
            zf_ref[pl.ds(start, size), :] = z
            sums = moments(z, sums)
    share(mids(0, 0), sums, index_of(0, 0))
    for copy in loads[2:] + kernels:
        copy.start()
    hc_ref[0] = jnp.zeros((line, 3 * middle), bf16)
    hc_ref[side + 1] = jnp.zeros((line, 3 * middle), bf16)
    empty = jnp.zeros((3 * middle, middle), bf16)
    for block in range(blocks):
        w2_ref[block, pl.ds(9 * middle, 3 * middle), 0:middle] = empty
        w2_ref[block, pl.ds(0, 3 * middle), middle : 2 * middle] = empty
    for copy in loads[2:] + kernels:
        copy.wait()
    for block in range(blocks):
        left_over = -mo_ref[pl.ds(block, 1), :]
        digits = []
        for _ in range(3):
            digits.append(left_over.astype(bf16).astype(f32))
            left_over = left_over - digits[-1]
        place_in = lax.broadcasted_iota(jnp.int32, (middle, channels), 0)
        below = jnp.zeros((middle, channels), f32)
        for i, digit in enumerate(digits):
            below = jnp.where(place_in == i, digit, below)
        we_ref[block, pl.ds(middle, middle), :] = below.astype(bf16)
    ones = (lax.broadcasted_iota(jnp.int32, (part, LANES), 1) < 3).astype(f32).astype(bf16)

    for block in range(blocks):
        mean_two = mm_ref[block, pl.ds(1, 1), :]
        scale1, offset1 = coefficients(
            collect(mids(block, 0), index_of(block, 0)),
            gm_ref[block, pl.ds(0, 1), :], bm_ref[block, pl.ds(0, 1), :],
            vm_ref[block, pl.ds(0, 1), :], count,
        )

        for t in range(tiles):
            z = zf_ref[pl.ds(t * part, part), :]
            h = jnp.maximum(z * scale1 + offset1, 0.0)
            left = pltpu.roll(h, images, 0).reshape(tall, line, middle)
            right = pltpu.roll(h, part - images, 0).reshape(tall, line, middle)
            left = jnp.where(place >= images, left, 0.0)
            right = jnp.where(place < line - images, right, 0.0)
            taps = (left, h.reshape(tall, line, middle), right)
            for i, tap in enumerate(taps):
                lanes = slice(i * middle, (i + 1) * middle)
                hc_ref[pl.ds(t * tall + 1, tall), :, lanes] = tap.astype(bf16)

        sums = zeros(middle)
        for t in range(tiles):
            v = hc_ref[pl.ds(t * tall, tall + 2)].reshape(tall // 2 + 1, 2, line, 3 * middle)
            lhs = jnp.concatenate(
                [v[:-1, 0], v[:-1, 1], v[1:, 0], v[1:, 1]], axis=-1
            ).reshape(part // 2, 12 * middle)
            z = jnp.dot(lhs, w2_ref[block], preferred_element_type=f32)
            for i in range(2):
                half = z[:, i * middle : (i + 1) * middle] - mean_two
                z_ref[pl.ds(t * (tall // 2), tall // 2), i] = half.reshape(
                    tall // 2, line, middle
                )
                sums = moments(half, sums)
        share(mids(block, 1), sums, index_of(block, 1))
        scale2, offset2 = coefficients(
            collect(mids(block, 1), index_of(block, 1)),
            gm_ref[block, pl.ds(1, 1), :], bm_ref[block, pl.ds(1, 1), :],
            vm_ref[block, pl.ds(1, 1), :], count,
        )

        for g in range(groups):
            wide = slice(g * width, (g + 1) * width)
            sums = zeros(width)
            for t in range(tiles):
                span = pl.ds(t * part, part)
                if g == 0:
                    z = zf_ref[span, :]
                    h = jnp.maximum((z * scale2 + offset2).astype(bf16), 0)
                    h_ref[span, :] = h
                else:
                    h = h_ref[span, :]
                lhs = jnp.concatenate([h, ones], axis=1)
                z = jnp.dot(lhs, we_ref[block, :, wide], preferred_element_type=f32)
                for c in range(per):
                    z3_ref[g * per + c, span, :] = z[:, c * LANES : (c + 1) * LANES]
                sums = moments(z, sums)
            share(outs(block, g), sums, index_of(block, 2 + g))

        last = block == blocks - 1
        if not last:
            mean_one = mm_ref[block + 1, pl.ds(0, 1), :]
            sums = zeros(middle)
        for g in range(groups):
            wide = slice(g * width, (g + 1) * width)
            coef = coefficients(
                collect(outs(block, g), index_of(block, 2 + g)),
                go_ref[pl.ds(block, 1), wide], bo_ref[pl.ds(block, 1), wide],
                vo_ref[pl.ds(block, 1), wide], count,
            )
            if last and g == groups - 1:
                for i in range(2):
                    coef_ref[pl.ds(i, 1), :] = coef[i]
                break
            for t in range(tiles):
                y = updated(t * part, part, g, coef)
                if last:
                    continue
                span = pl.ds(t * part, part)
                y = jnp.concatenate(y, axis=1)
                z = jnp.dot(y, wr_ref[block + 1, wide, :], preferred_element_type=f32)
                z = z + zf_ref[span, :] if g else z - mean_one
                zf_ref[span, :] = z
                if g == groups - 1:
                    sums = moments(z, sums)
        if not last:
            share(mids(block + 1, 0), sums, index_of(block + 1, 0))

    for block in range(blocks):
        for i in range(2):
            slots(mids(block, i), index_of(block, i)).wait_send()
        for g in range(groups):
            slots(outs(block, g), index_of(block, 2 + g)).wait_send()


def last_kernel(pieces, x_ref, z3_ref, coef_ref, o_ref, y_ref, out_sem, old_sem):
    slabs = x_ref.shape[0]
    pixels, images, channels = o_ref.shape
    part = pixels // pieces * images
    per = coef_ref.shape[1] // LANES
    done = slabs - per
    flat_ref = o_ref.reshape(pixels * images, channels)

    def old_copy(c):
        return pltpu.make_async_copy(
            x_ref.at[c], flat_ref.at[:, pl.ds(c * LANES, LANES)], old_sem.at[c]
        )

    def slab_copy(t, c):
        span = pl.ds(t * part, part)
        far = flat_ref.at[span, pl.ds((done + c) * LANES, LANES)]
        return pltpu.make_async_copy(y_ref.at[c, span], far, out_sem.at[t, c])

    for c in range(done):
        old_copy(c).start()

    def step(t, carry):
        span = pl.ds(pl.multiple_of(t * part, 16), part)
        for c in range(per):
            lanes = slice(c * LANES, (c + 1) * LANES)
            scale, offset = (coef_ref[pl.ds(i, 1), lanes] for i in range(2))
            z = z3_ref[done + c, span, :] * scale + offset
            y = z.astype(bf16) + x_ref[done + c, span, :]
            y_ref[c, span, :] = jnp.maximum(y, 0)
            slab_copy(t, c).start()
        return carry

    lax.fori_loop(0, pieces, step, 0)
    for c in range(done):
        old_copy(c).wait()
    for t in range(pieces):
        for c in range(per):
            slab_copy(t, c).wait()


def local(mesh_rows, mesh_cols, images, w_reduce, w_spatial, w_expand, *params):
    held, side, _, channels = images.shape
    blocks, _, middle = w_reduce.shape
    devices = mesh_rows * mesh_cols
    count = float(held * side * side * devices)
    tiles = next(t for t in (TILES, 2, 1) if side % (2 * t) == 0)
    slabs = channels // LANES
    pixels = side * side
    loads_in = next(t for t in (4, 2, 1) if pixels * held % (16 * t) == 0)
    width = group_width(channels)
    groups = channels // width
    vmem = pl.BlockSpec(memory_space=pltpu.VMEM)
    anywhere = pl.BlockSpec(memory_space=pltpu.HBM)
    turned = images.transpose(1, 2, 0, 3).reshape(pixels, held, channels)
    taps = w_spatial.reshape(blocks, 9 * middle, middle)
    operands = [
        pltpu.with_memory_space_constraint(a, pltpu.HBM)
        for a in (turned, w_reduce, taps, w_expand, *params)
    ]
    x, z3, coef = pl.pallas_call(
        functools.partial(main_kernel, mesh_rows, mesh_cols, count, side, tiles, loads_in),
        out_shape=(
            jax.ShapeDtypeStruct((slabs, pixels * held, LANES), bf16),
            jax.ShapeDtypeStruct((slabs, pixels * held, LANES), f32),
            jax.ShapeDtypeStruct((2, width), f32),
        ),
        in_specs=[anywhere] * 12,
        out_specs=(vmem, vmem, vmem),
        scratch_shapes=[
            pltpu.VMEM((side // 2, 2, side * held, middle), f32),
            pltpu.VMEM((pixels * held, middle), bf16),
            pltpu.VMEM((side + 2, side * held, 3 * middle), bf16),
            pltpu.VMEM((blocks, 12 * middle, 2 * middle), bf16),
            pltpu.VMEM((2 * blocks, devices, 2, middle), f32),
            pltpu.VMEM((blocks, groups, devices, 2, width), f32),
            pltpu.VMEM(w_reduce.shape, bf16),
            pltpu.VMEM((blocks, 2 * middle, channels), bf16),
            *(pltpu.VMEM(p.shape, f32) for p in params),
            pltpu.SemaphoreType.DMA((loads_in, slabs)),
            pltpu.SemaphoreType.DMA((11,)),
            pltpu.SemaphoreType.DMA((blocks, 2)),
            pltpu.SemaphoreType.DMA(((2 + groups) * blocks,)),
            pltpu.SemaphoreType.DMA(((2 + groups) * blocks,)),
        ],
        compiler_params=pltpu.CompilerParams(
            collective_id=0, has_side_effects=True, vmem_limit_bytes=LIMIT * 1024 * 1024
        ),
        name="bottlenecks",
    )(*operands)
    pieces = side // 4 if side % 4 == 0 else 1
    out = pl.pallas_call(
        functools.partial(last_kernel, pieces),
        out_shape=jax.ShapeDtypeStruct((pixels, held, channels), bf16),
        in_specs=[vmem] * 3,
        out_specs=anywhere,
        scratch_shapes=[
            pltpu.VMEM((width // LANES, pixels * held, LANES), bf16),
            pltpu.SemaphoreType.DMA((pieces, width // LANES)),
            pltpu.SemaphoreType.DMA((slabs,)),
        ],
        compiler_params=pltpu.CompilerParams(vmem_limit_bytes=16 * 1024 * 1024),
        name="finish",
    )(x, z3, coef)
    return out.reshape(side, side, held, channels).transpose(2, 0, 1, 3)


TILES = 2
LIMIT = 32


def solution(mesh):
    spec = P(("row", "col"), None, None, None)
    return jax.shard_map(
        functools.partial(local, mesh.shape["row"], mesh.shape["col"]),
        mesh=mesh,
        in_specs=(spec,) + (P(),) * 11,
        out_specs=spec,
        check_vma=False,
    )
```

```python
import functools

import jax
import jax.numpy as jnp
from jax import lax
from jax.experimental import pallas as pl
from jax.experimental.pallas import tpu as pltpu
from jax.sharding import PartitionSpec as P

epsilon = 1e-05
ratio_max = 3.0
shift_max = 5.0
MESH = pl.DeviceIdType.MESH
LANES = 128
f32 = jnp.float32
bf16 = jnp.bfloat16


def coefficients(total, gain, bias, run_var, count):
    mean_offset = total[0:1] / count
    variance = jnp.maximum(total[1:2] / count - mean_offset * mean_offset, 0.0)
    sigma = jnp.sqrt(variance + epsilon)
    run_sigma = jnp.sqrt(run_var + epsilon)
    ratio = jnp.clip(sigma / run_sigma, 1.0 / ratio_max, ratio_max)
    shift = jnp.clip(mean_offset / run_sigma, -shift_max, shift_max)
    scale = gain * (ratio / sigma)
    return scale, gain * shift + bias - mean_offset * scale


def flipped(index, bits):
    out, bit = index, 1
    while bit <= bits:
        if bits & bit:
            out = out + bit - 2 * bit * lax.rem(lax.div(index, bit), 2)
        bit *= 2
    return out


def tree_sum(parts):
    while len(parts) > 1:
        half = [a + b for a, b in zip(parts[0::2], parts[1::2])]
        parts = half + ([parts[-1]] if len(parts) % 2 else [])
    return parts[0]


def group_width(channels):
    return 2 * LANES if channels % (2 * LANES) == 0 else channels


def main_kernel(
    rows,
    cols,
    count,
    side,
    tiles,
    loads_in,
    img_ref,
    wr_hbm,
    ws_hbm,
    we_hbm,
    gm_hbm,
    bm_hbm,
    mm_hbm,
    vm_hbm,
    go_hbm,
    bo_hbm,
    mo_hbm,
    vo_hbm,
    x_ref,
    z3_ref,
    coef_ref,
    z_ref,
    hc_ref,
    w2_ref,
    mid_buf,
    out_buf,
    wr_ref,
    we_ref,
    gm_ref,
    bm_ref,
    mm_ref,
    vm_ref,
    go_ref,
    bo_ref,
    mo_ref,
    vo_ref,
    in_sem,
    par_sem,
    tap_sem,
    send_sem,
    recv_sem,
):
    devices = rows * cols
    pixels, images, channels = img_ref.shape
    blocks, _, middle = wr_ref.shape
    slabs = channels // LANES
    width = group_width(channels)
    groups = channels // width
    per = width // LANES
    line = side * images
    tall = side // tiles
    part = tall * line
    total_rows = pixels * images
    my_row, my_col = lax.axis_index("row"), lax.axis_index("col")
    me = my_row * cols + my_col
    flat_ref = img_ref.reshape(total_rows, channels)
    zf_ref = z_ref.reshape(total_rows, middle)
    piece = total_rows // loads_in
    chunk = next(16 * k for k in (14, 7, 4, 2, 1) if total_rows % (16 * k) == 0)

    def slab_copy(t, c):
        span = pl.ds(t * piece, piece)
        far = flat_ref.at[span, pl.ds(c * LANES, LANES)]
        return pltpu.make_async_copy(far, x_ref.at[c, span], in_sem.at[t])

    pairs = (
        (wr_hbm.at[0], wr_ref.at[0]), (mm_hbm, mm_ref), (we_hbm, we_ref.at[:, pl.ds(0, middle)]), (gm_hbm, gm_ref),
        (bm_hbm, bm_ref), (vm_hbm, vm_ref), (go_hbm, go_ref), (bo_hbm, bo_ref),
        (mo_hbm, mo_ref), (vo_hbm, vo_ref),
    )
    loads = [pltpu.make_async_copy(a, b, par_sem.at[i]) for i, (a, b) in enumerate(pairs)]
    if blocks > 1:
        rest = pl.ds(1, blocks - 1)
        loads.append(pltpu.make_async_copy(wr_hbm.at[rest], wr_ref.at[rest], par_sem.at[len(pairs)]))
    kernels = [
        pltpu.make_async_copy(
            ws_hbm.at[block],
            w2_ref.at[block, pl.ds(3 * i * middle, 9 * middle), pl.ds(i * middle, middle)],
            tap_sem.at[block, i],
        )
        for block in range(blocks)
        for i in range(2)
    ]
    barrier = pltpu.get_barrier_semaphore()

    def to_all(act):
        if devices <= 64:
            if rows & (rows - 1) == 0 and cols & (cols - 1) == 0:
                far_rows = [flipped(my_row, i) for i in range(rows)]
                far_cols = [flipped(my_col, i) for i in range(cols)]
            else:
                far_rows = [lax.rem(my_row + i, rows) for i in range(rows)]
                far_cols = [lax.rem(my_col + i, cols) for i in range(cols)]
            for j in range(cols - 1, -1, -1):
                for i in range(rows - 1, -1, -1):
                    if i or j:
                        act((far_rows[i], far_cols[j]))
        else:

            def step(i, c):
                other = lax.rem(me + i, devices)
                act((lax.div(other, cols), lax.rem(other, cols)))
                return c

            lax.fori_loop(1, devices, step, 0)

    for copy in loads[:2]:
        copy.start()
    to_all(
        lambda there: pl.semaphore_signal(
            barrier, inc=1, device_id=there, device_id_type=MESH
        )
    )

    for t in range(loads_in):
        for c in range(slabs):
            slab_copy(t, c).start()

    def slots(ref, index):
        others = ref.at[pl.ds(0, devices - 1)]
        return pltpu.make_async_remote_copy(
            src_ref=others,
            dst_ref=others,
            send_sem=send_sem.at[index],
            recv_sem=recv_sem.at[index],
            device_id=(lax.rem(my_row + 1, rows), my_col),
            device_id_type=MESH,
        )

    def share(ref, sums, index):
        for i in range(2):
            ref[me, pl.ds(i, 1), :] = jnp.sum(sums[i], axis=0, keepdims=True)
        if index == 0:
            pl.semaphore_wait(barrier, devices - 1)

        def send(there):
            pltpu.make_async_remote_copy(
                src_ref=ref.at[me],
                dst_ref=ref.at[me],
                send_sem=send_sem.at[index],
                recv_sem=recv_sem.at[index],
                device_id=there,
                device_id_type=MESH,
            ).start()

        to_all(send)

    def collect(ref, index):
        exchange = slots(ref, index)
        exchange.wait_send()
        exchange.wait_recv()
        if devices <= 64:
            return tree_sum([ref[d] for d in range(devices)])
        return jnp.sum(ref[...], axis=0)

    def moments(d, sums):
        d = d.reshape(-1, 16, d.shape[-1])
        return sums[0] + jnp.sum(d, axis=0), sums[1] + jnp.sum(d * d, axis=0)

    def zeros(c):
        return (jnp.zeros((16, c), f32), jnp.zeros((16, c), f32))

    for copy in loads[:2]:
        copy.wait()
    place = lax.broadcasted_iota(jnp.int32, (1, line, 1), 1)

    def updated(start, size, g, coef, keep):
        scale, offset = coef
        new = []
        for c in range(per):
            lanes = slice(c * LANES, (c + 1) * LANES)
            slab = g * per + c
            span = pl.ds(start, size)
            z = z3_ref[slab, span, :] * scale[:, lanes] + offset[:, lanes]
            y = jnp.maximum(z.astype(bf16) + x_ref[slab, span, :], 0)
            if keep:
                x_ref[slab, span, :] = y
            new.append(y)
        return new

    def halves(start, size):
        first = (size // 2 + 15) // 16 * 16
        return ((start, first), (start + first, size - first))

    per_block = 2 + groups

    def index_of(block, stage):
        return per_block * block + stage

    mids = lambda block, i: mid_buf.at[2 * block + i]
    outs = lambda block, g: out_buf.at[block, g]

    sums = zeros(middle)
    mean_one = mm_ref[0, pl.ds(0, 1), :]
    for t in range(loads_in):
        tile = x_ref.at[:, pl.ds(t * piece, piece)]
        pltpu.make_async_copy(tile, tile, in_sem.at[t]).wait()
        for start, size in halves(t * piece, piece):
            x = jnp.concatenate([x_ref[c, pl.ds(start, size), :] for c in range(slabs)], axis=1)
            z = jnp.dot(x, wr_ref[0], preferred_element_type=f32) - mean_one
            zf_ref[pl.ds(start, size), :] = z
            sums = moments(z, sums)
    share(mids(0, 0), sums, index_of(0, 0))
    for copy in loads[2:] + kernels:
        copy.start()
    hc_ref[0] = jnp.zeros((line, 3 * middle), bf16)
    hc_ref[side + 1] = jnp.zeros((line, 3 * middle), bf16)
    empty = jnp.zeros((3 * middle, middle), bf16)
    for block in range(blocks):
        w2_ref[block, pl.ds(9 * middle, 3 * middle), 0:middle] = empty
        w2_ref[block, pl.ds(0, 3 * middle), middle : 2 * middle] = empty
    for copy in loads[2:] + kernels:
        copy.wait()
    for block in range(blocks):
        left_over = -mo_ref[pl.ds(block, 1), :]
        digits = []
        for _ in range(3):
            digits.append(left_over.astype(bf16).astype(f32))
            left_over = left_over - digits[-1]
        place_in = lax.broadcasted_iota(jnp.int32, (middle, channels), 0)
        below = jnp.zeros((middle, channels), f32)
        for i, digit in enumerate(digits):
            below = jnp.where(place_in == i, digit, below)
        we_ref[block, pl.ds(middle, middle), :] = below.astype(bf16)
    ones = (lax.broadcasted_iota(jnp.int32, (part, LANES), 1) < 3).astype(f32).astype(bf16)

    for block in range(blocks):
        mean_two = mm_ref[block, pl.ds(1, 1), :]
        scale1, offset1 = coefficients(
            collect(mids(block, 0), index_of(block, 0)),
            gm_ref[block, pl.ds(0, 1), :], bm_ref[block, pl.ds(0, 1), :],
            vm_ref[block, pl.ds(0, 1), :], count,
        )

        for t in range(tiles):
            z = zf_ref[pl.ds(t * part, part), :]
            h = jnp.maximum(z * scale1 + offset1, 0.0)
            left = pltpu.roll(h, images, 0).reshape(tall, line, middle)
            right = pltpu.roll(h, part - images, 0).reshape(tall, line, middle)
            left = jnp.where(place >= images, left, 0.0)
            right = jnp.where(place < line - images, right, 0.0)
            taps = (left, h.reshape(tall, line, middle), right)
            for i, tap in enumerate(taps):
                lanes = slice(i * middle, (i + 1) * middle)
                hc_ref[pl.ds(t * tall + 1, tall), :, lanes] = tap.astype(bf16)

        sums = zeros(middle)
        for t in range(tiles):
            v = hc_ref[pl.ds(t * tall, tall + 2)].reshape(tall // 2 + 1, 2, line, 3 * middle)
            lhs = jnp.concatenate(
                [v[:-1, 0], v[:-1, 1], v[1:, 0], v[1:, 1]], axis=-1
            ).reshape(part // 2, 12 * middle)
            z = jnp.dot(lhs, w2_ref[block], preferred_element_type=f32)
            for i in range(2):
                half = z[:, i * middle : (i + 1) * middle] - mean_two
                z_ref[pl.ds(t * (tall // 2), tall // 2), i] = half.reshape(
                    tall // 2, line, middle
                )
                sums = moments(half, sums)
        share(mids(block, 1), sums, index_of(block, 1))
        scale2, offset2 = coefficients(
            collect(mids(block, 1), index_of(block, 1)),
            gm_ref[block, pl.ds(1, 1), :], bm_ref[block, pl.ds(1, 1), :],
            vm_ref[block, pl.ds(1, 1), :], count,
        )

        for g in range(groups):
            wide = slice(g * width, (g + 1) * width)
            sums = zeros(width)
            for t in range(tiles):
                span = pl.ds(t * part, part)
                h = zf_ref[span, :]
                if g == 0:
                    h = jnp.maximum(h * scale2 + offset2, 0.0)
                    zf_ref[span, :] = h
                h = h.astype(bf16)
                lhs = jnp.concatenate([h, ones], axis=1)
                z = jnp.dot(lhs, we_ref[block, :, wide], preferred_element_type=f32)
                for c in range(per):
                    z3_ref[g * per + c, span, :] = z[:, c * LANES : (c + 1) * LANES]
                sums = moments(z, sums)
            share(outs(block, g), sums, index_of(block, 2 + g))

        last = block == blocks - 1
        if not last:
            mean_one = mm_ref[block + 1, pl.ds(0, 1), :]
            sums = zeros(middle)
        coefs = []
        for g in range(groups):
            wide = slice(g * width, (g + 1) * width)
            coef = coefficients(
                collect(outs(block, g), index_of(block, 2 + g)),
                go_ref[pl.ds(block, 1), wide], bo_ref[pl.ds(block, 1), wide],
                vo_ref[pl.ds(block, 1), wide], count,
            )
            coefs.append(coef)
            if last and g == groups - 1:
                for i in range(2):
                    coef_ref[pl.ds(i, 1), :] = coef[i]
                break
            for t in range(tiles):
                y = updated(t * part, part, g, coef, last)
                if last:
                    continue
                span = pl.ds(t * part, part)
                y = jnp.concatenate(y, axis=1)
                z = jnp.dot(y, wr_ref[block + 1, wide, :], preferred_element_type=f32)
                z = z + zf_ref[span, :] if g else z - mean_one
                zf_ref[span, :] = z
                if g == groups - 1:
                    sums = moments(z, sums)
        if not last:
            share(mids(block + 1, 0), sums, index_of(block + 1, 0))

            def keep(t, carry):
                for g in range(groups):
                    updated(pl.multiple_of(t * chunk, 16), chunk, g, coefs[g], True)
                return carry

            lax.fori_loop(0, total_rows // chunk, keep, 0)


def last_kernel(pieces, x_ref, z3_ref, coef_ref, o_ref, y_ref, out_sem, old_sem):
    slabs = x_ref.shape[0]
    pixels, images, channels = o_ref.shape
    part = pixels // pieces * images
    per = coef_ref.shape[1] // LANES
    done = slabs - per
    flat_ref = o_ref.reshape(pixels * images, channels)

    def old_copy(c):
        return pltpu.make_async_copy(
            x_ref.at[c], flat_ref.at[:, pl.ds(c * LANES, LANES)], old_sem.at[c]
        )

    def slab_copy(t, c):
        span = pl.ds(t * part, part)
        far = flat_ref.at[span, pl.ds((done + c) * LANES, LANES)]
        return pltpu.make_async_copy(y_ref.at[c, span], far, out_sem.at[t, c])

    for c in range(done):
        old_copy(c).start()

    def step(t, carry):
        span = pl.ds(pl.multiple_of(t * part, 16), part)
        for c in range(per):
            lanes = slice(c * LANES, (c + 1) * LANES)
            scale, offset = (coef_ref[pl.ds(i, 1), lanes] for i in range(2))
            z = z3_ref[done + c, span, :] * scale + offset
            y = z.astype(bf16) + x_ref[done + c, span, :]
            y_ref[c, span, :] = jnp.maximum(y, 0)
            slab_copy(t, c).start()
        return carry

    lax.fori_loop(0, pieces, step, 0)
    for c in range(done):
        old_copy(c).wait()
    for t in range(pieces):
        for c in range(per):
            slab_copy(t, c).wait()


def local(mesh_rows, mesh_cols, images, w_reduce, w_spatial, w_expand, *params):
    held, side, _, channels = images.shape
    blocks, _, middle = w_reduce.shape
    devices = mesh_rows * mesh_cols
    count = float(held * side * side * devices)
    tiles = next(t for t in (TILES, 2, 1) if side % (2 * t) == 0)
    slabs = channels // LANES
    pixels = side * side
    loads_in = next(t for t in (4, 2, 1) if pixels * held % (16 * t) == 0)
    width = group_width(channels)
    groups = channels // width
    vmem = pl.BlockSpec(memory_space=pltpu.VMEM)
    anywhere = pl.BlockSpec(memory_space=pltpu.HBM)
    turned = images.transpose(1, 2, 0, 3).reshape(pixels, held, channels)
    taps = w_spatial.reshape(blocks, 9 * middle, middle)
    operands = [
        pltpu.with_memory_space_constraint(a, pltpu.HBM)
        for a in (turned, w_reduce, taps, w_expand, *params)
    ]
    x, z3, coef = pl.pallas_call(
        functools.partial(main_kernel, mesh_rows, mesh_cols, count, side, tiles, loads_in),
        out_shape=(
            jax.ShapeDtypeStruct((slabs, pixels * held, LANES), bf16),
            jax.ShapeDtypeStruct((slabs, pixels * held, LANES), f32),
            jax.ShapeDtypeStruct((2, width), f32),
        ),
        in_specs=[anywhere] * 12,
        out_specs=(vmem, vmem, vmem),
        scratch_shapes=[
            pltpu.VMEM((side // 2, 2, side * held, middle), f32),
            pltpu.VMEM((side + 2, side * held, 3 * middle), bf16),
            pltpu.VMEM((blocks, 12 * middle, 2 * middle), bf16),
            pltpu.VMEM((2 * blocks, devices, 2, middle), f32),
            pltpu.VMEM((blocks, groups, devices, 2, width), f32),
            pltpu.VMEM(w_reduce.shape, bf16),
            pltpu.VMEM((blocks, 2 * middle, channels), bf16),
            *(pltpu.VMEM(p.shape, f32) for p in params),
            pltpu.SemaphoreType.DMA((loads_in,)),
            pltpu.SemaphoreType.DMA((11,)),
            pltpu.SemaphoreType.DMA((blocks, 2)),
            pltpu.SemaphoreType.DMA(((2 + groups) * blocks,)),
            pltpu.SemaphoreType.DMA(((2 + groups) * blocks,)),
        ],
        compiler_params=pltpu.CompilerParams(
            collective_id=0, has_side_effects=True, vmem_limit_bytes=LIMIT * 1024 * 1024
        ),
        name="bottlenecks",
    )(*operands)
    pieces = side // 4 if side % 4 == 0 else 1
    out = pl.pallas_call(
        functools.partial(last_kernel, pieces),
        out_shape=jax.ShapeDtypeStruct((pixels, held, channels), bf16),
        in_specs=[vmem] * 3,
        out_specs=anywhere,
        scratch_shapes=[
            pltpu.VMEM((width // LANES, pixels * held, LANES), bf16),
            pltpu.SemaphoreType.DMA((pieces, width // LANES)),
            pltpu.SemaphoreType.DMA((slabs,)),
        ],
        compiler_params=pltpu.CompilerParams(vmem_limit_bytes=16 * 1024 * 1024),
        name="finish",
    )(x, z3, coef)
    return out.reshape(side, side, held, channels).transpose(2, 0, 1, 3)


TILES = 2
LIMIT = 32


def solution(mesh):
    spec = P(("row", "col"), None, None, None)
    return jax.shard_map(
        functools.partial(local, mesh.shape["row"], mesh.shape["col"]),
        mesh=mesh,
        in_specs=(spec,) + (P(),) * 11,
        out_specs=spec,
        check_vma=False,
    )
```

```python
import functools

import jax
import jax.numpy as jnp
from jax import lax
from jax.experimental import pallas as pl
from jax.experimental.pallas import tpu as pltpu
from jax.sharding import PartitionSpec as P

epsilon = 1e-05
ratio_max = 3.0
shift_max = 5.0
MESH = pl.DeviceIdType.MESH
LANES = 128
f32 = jnp.float32
bf16 = jnp.bfloat16


def coefficients(total, gain, bias, run_var, count):
    mean_offset = total[0:1] * (1.0 / count)
    variance = jnp.maximum(total[1:2] * (1.0 / count) - mean_offset * mean_offset, 0.0)
    inverse = lax.rsqrt(variance + epsilon)
    run_inverse = lax.rsqrt(run_var + epsilon)
    scale = gain * jnp.clip(run_inverse, inverse * (1.0 / ratio_max), inverse * ratio_max)
    shift = jnp.clip(mean_offset * run_inverse, -shift_max, shift_max)
    return scale, gain * shift + bias - mean_offset * scale


def flipped(index, bits):
    out, bit = index, 1
    while bit <= bits:
        if bits & bit:
            out = out + bit - 2 * bit * lax.rem(lax.div(index, bit), 2)
        bit *= 2
    return out


def tree_sum(parts):
    while len(parts) > 1:
        half = [a + b for a, b in zip(parts[0::2], parts[1::2])]
        parts = half + ([parts[-1]] if len(parts) % 2 else [])
    return parts[0]


def group_width(channels):
    return 2 * LANES if channels % (2 * LANES) == 0 else channels


def main_kernel(
    rows,
    cols,
    count,
    side,
    tiles,
    loads_in,
    img_ref,
    wr_hbm,
    ws_hbm,
    we_hbm,
    gm_hbm,
    bm_hbm,
    mm_hbm,
    vm_hbm,
    go_hbm,
    bo_hbm,
    mo_hbm,
    vo_hbm,
    x_ref,
    z3_ref,
    coef_ref,
    z_ref,
    hc_ref,
    w2_ref,
    mid_buf,
    out_buf,
    wr_ref,
    we_ref,
    gm_ref,
    bm_ref,
    mm_ref,
    vm_ref,
    go_ref,
    bo_ref,
    mo_ref,
    vo_ref,
    in_sem,
    par_sem,
    tap_sem,
    send_sem,
    recv_sem,
):
    devices = rows * cols
    pixels, images, channels = img_ref.shape
    blocks, _, middle = wr_ref.shape
    slabs = channels // LANES
    width = group_width(channels)
    groups = channels // width
    per = width // LANES
    line = side * images
    tall = side // tiles
    part = tall * line
    total_rows = pixels * images
    my_row, my_col = lax.axis_index("row"), lax.axis_index("col")
    me = my_row * cols + my_col
    flat_ref = img_ref.reshape(total_rows, channels)
    zf_ref = z_ref.reshape(total_rows, middle)
    piece = total_rows // loads_in
    chunk = next(16 * k for k in (14, 7, 4, 2, 1) if total_rows % (16 * k) == 0)

    def slab_copy(t, c):
        span = pl.ds(t * piece, piece)
        far = flat_ref.at[span, pl.ds(c * LANES, LANES)]
        return pltpu.make_async_copy(far, x_ref.at[c, span], in_sem.at[t])

    pairs = (
        (wr_hbm.at[0], wr_ref.at[0]), (mm_hbm, mm_ref), (we_hbm, we_ref.at[:, pl.ds(0, middle)]), (gm_hbm, gm_ref),
        (bm_hbm, bm_ref), (vm_hbm, vm_ref), (go_hbm, go_ref), (bo_hbm, bo_ref),
        (mo_hbm, mo_ref), (vo_hbm, vo_ref),
    )
    loads = [pltpu.make_async_copy(a, b, par_sem.at[i]) for i, (a, b) in enumerate(pairs)]
    if blocks > 1:
        rest = pl.ds(1, blocks - 1)
        loads.append(pltpu.make_async_copy(wr_hbm.at[rest], wr_ref.at[rest], par_sem.at[len(pairs)]))
    kernels = [
        pltpu.make_async_copy(
            ws_hbm.at[block],
            w2_ref.at[block, pl.ds(3 * i * middle, 9 * middle), pl.ds(i * middle, middle)],
            tap_sem.at[block, i],
        )
        for block in range(blocks)
        for i in range(2)
    ]
    barrier = pltpu.get_barrier_semaphore()

    def to_all(act):
        if devices <= 64:
            if rows & (rows - 1) == 0 and cols & (cols - 1) == 0:
                far_rows = [flipped(my_row, i) for i in range(rows)]
                far_cols = [flipped(my_col, i) for i in range(cols)]
            else:
                far_rows = [lax.rem(my_row + i, rows) for i in range(rows)]
                far_cols = [lax.rem(my_col + i, cols) for i in range(cols)]
            for j in range(cols - 1, -1, -1):
                for i in range(rows - 1, -1, -1):
                    if i or j:
                        act((far_rows[i], far_cols[j]))
        else:

            def step(i, c):
                other = lax.rem(me + i, devices)
                act((lax.div(other, cols), lax.rem(other, cols)))
                return c

            lax.fori_loop(1, devices, step, 0)

    for copy in loads[:2]:
        copy.start()
    to_all(
        lambda there: pl.semaphore_signal(
            barrier, inc=1, device_id=there, device_id_type=MESH
        )
    )

    for t in range(loads_in):
        for c in range(slabs):
            slab_copy(t, c).start()

    def slots(ref, index):
        others = ref.at[pl.ds(0, devices - 1)]
        return pltpu.make_async_remote_copy(
            src_ref=others,
            dst_ref=others,
            send_sem=send_sem.at[index],
            recv_sem=recv_sem.at[index],
            device_id=(lax.rem(my_row + 1, rows), my_col),
            device_id_type=MESH,
        )

    def share(ref, sums, index):
        for i in range(2):
            ref[me, pl.ds(i, 1), :] = jnp.sum(sums[i], axis=0, keepdims=True)
        if index == 0:
            pl.semaphore_wait(barrier, devices - 1)

        def send(there):
            pltpu.make_async_remote_copy(
                src_ref=ref.at[me],
                dst_ref=ref.at[me],
                send_sem=send_sem.at[index],
                recv_sem=recv_sem.at[index],
                device_id=there,
                device_id_type=MESH,
            ).start()

        to_all(send)

    def collect(ref, index):
        exchange = slots(ref, index)
        exchange.wait_send()
        exchange.wait_recv()
        if devices <= 64:
            return tree_sum([ref[d] for d in range(devices)])
        return jnp.sum(ref[...], axis=0)

    def moments(d, sums):
        d = d.reshape(-1, 16, d.shape[-1])
        return sums[0] + jnp.sum(d, axis=0), sums[1] + jnp.sum(d * d, axis=0)

    def zeros(c):
        return (jnp.zeros((16, c), f32), jnp.zeros((16, c), f32))

    for copy in loads[:2]:
        copy.wait()
    place = lax.broadcasted_iota(jnp.int32, (1, line, 1), 1)

    def updated(start, size, g, coef, keep):
        scale, offset = coef
        new = []
        for c in range(per):
            lanes = slice(c * LANES, (c + 1) * LANES)
            slab = g * per + c
            span = pl.ds(start, size)
            z = z3_ref[slab, span, :] * scale[:, lanes] + offset[:, lanes]
            y = jnp.maximum(z.astype(bf16) + x_ref[slab, span, :], 0)
            if keep:
                x_ref[slab, span, :] = y
            new.append(y)
        return new

    def halves(start, size):
        first = (size // 2 + 15) // 16 * 16
        return ((start, first), (start + first, size - first))

    per_block = 2 + groups

    def index_of(block, stage):
        return per_block * block + stage

    mids = lambda block, i: mid_buf.at[2 * block + i]
    outs = lambda block, g: out_buf.at[block, g]

    sums = zeros(middle)
    mean_one = mm_ref[0, pl.ds(0, 1), :]
    for t in range(loads_in):
        tile = x_ref.at[:, pl.ds(t * piece, piece)]
        pltpu.make_async_copy(tile, tile, in_sem.at[t]).wait()
        for start, size in halves(t * piece, piece):
            x = jnp.concatenate([x_ref[c, pl.ds(start, size), :] for c in range(slabs)], axis=1)
            z = jnp.dot(x, wr_ref[0], preferred_element_type=f32) - mean_one
            zf_ref[pl.ds(start, size), :] = z
            sums = moments(z, sums)
    share(mids(0, 0), sums, index_of(0, 0))
    for copy in loads[2:] + kernels:
        copy.start()
    hc_ref[0] = jnp.zeros((line, 3 * middle), bf16)
    hc_ref[side + 1] = jnp.zeros((line, 3 * middle), bf16)
    empty = jnp.zeros((3 * middle, middle), bf16)
    for block in range(blocks):
        w2_ref[block, pl.ds(9 * middle, 3 * middle), 0:middle] = empty
        w2_ref[block, pl.ds(0, 3 * middle), middle : 2 * middle] = empty
    for copy in loads[2:] + kernels:
        copy.wait()
    for block in range(blocks):
        left_over = -mo_ref[pl.ds(block, 1), :]
        digits = []
        for _ in range(3):
            digits.append(left_over.astype(bf16).astype(f32))
            left_over = left_over - digits[-1]
        place_in = lax.broadcasted_iota(jnp.int32, (middle, channels), 0)
        below = jnp.zeros((middle, channels), f32)
        for i, digit in enumerate(digits):
            below = jnp.where(place_in == i, digit, below)
        we_ref[block, pl.ds(middle, middle), :] = below.astype(bf16)
    ones = (lax.broadcasted_iota(jnp.int32, (part, LANES), 1) < 3).astype(f32).astype(bf16)

    for block in range(blocks):
        mean_two = mm_ref[block, pl.ds(1, 1), :]
        scale1, offset1 = coefficients(
            collect(mids(block, 0), index_of(block, 0)),
            gm_ref[block, pl.ds(0, 1), :], bm_ref[block, pl.ds(0, 1), :],
            vm_ref[block, pl.ds(0, 1), :], count,
        )

        for t in range(tiles):
            z = zf_ref[pl.ds(t * part, part), :]
            h = jnp.maximum(z * scale1 + offset1, 0.0)
            left = pltpu.roll(h, images, 0).reshape(tall, line, middle)
            right = pltpu.roll(h, part - images, 0).reshape(tall, line, middle)
            left = jnp.where(place >= images, left, 0.0)
            right = jnp.where(place < line - images, right, 0.0)
            taps = (left, h.reshape(tall, line, middle), right)
            for i, tap in enumerate(taps):
                lanes = slice(i * middle, (i + 1) * middle)
                hc_ref[pl.ds(t * tall + 1, tall), :, lanes] = tap.astype(bf16)

        sums = zeros(middle)
        for t in range(tiles):
            v = hc_ref[pl.ds(t * tall, tall + 2)].reshape(tall // 2 + 1, 2, line, 3 * middle)
            lhs = jnp.concatenate(
                [v[:-1, 0], v[:-1, 1], v[1:, 0], v[1:, 1]], axis=-1
            ).reshape(part // 2, 12 * middle)
            z = jnp.dot(lhs, w2_ref[block], preferred_element_type=f32)
            for i in range(2):
                half = z[:, i * middle : (i + 1) * middle] - mean_two
                z_ref[pl.ds(t * (tall // 2), tall // 2), i] = half.reshape(
                    tall // 2, line, middle
                )
                sums = moments(half, sums)
        share(mids(block, 1), sums, index_of(block, 1))
        scale2, offset2 = coefficients(
            collect(mids(block, 1), index_of(block, 1)),
            gm_ref[block, pl.ds(1, 1), :], bm_ref[block, pl.ds(1, 1), :],
            vm_ref[block, pl.ds(1, 1), :], count,
        )

        for g in range(groups):
            wide = slice(g * width, (g + 1) * width)
            sums = zeros(width)
            for t in range(tiles):
                span = pl.ds(t * part, part)
                h = zf_ref[span, :]
                if g == 0:
                    h = jnp.maximum(h * scale2 + offset2, 0.0)
                    zf_ref[span, :] = h
                h = h.astype(bf16)
                lhs = jnp.concatenate([h, ones], axis=1)
                z = jnp.dot(lhs, we_ref[block, :, wide], preferred_element_type=f32)
                for c in range(per):
                    z3_ref[g * per + c, span, :] = z[:, c * LANES : (c + 1) * LANES]
                sums = moments(z, sums)
            share(outs(block, g), sums, index_of(block, 2 + g))

        last = block == blocks - 1
        if not last:
            mean_one = mm_ref[block + 1, pl.ds(0, 1), :]
            sums = zeros(middle)
        coefs = []
        for g in range(groups):
            wide = slice(g * width, (g + 1) * width)
            coef = coefficients(
                collect(outs(block, g), index_of(block, 2 + g)),
                go_ref[pl.ds(block, 1), wide], bo_ref[pl.ds(block, 1), wide],
                vo_ref[pl.ds(block, 1), wide], count,
            )
            coefs.append(coef)
            if last and g == groups - 1:
                for i in range(2):
                    coef_ref[pl.ds(i, 1), :] = coef[i]
                break
            for t in range(tiles):
                y = updated(t * part, part, g, coef, last)
                if last:
                    continue
                span = pl.ds(t * part, part)
                y = jnp.concatenate(y, axis=1)
                z = jnp.dot(y, wr_ref[block + 1, wide, :], preferred_element_type=f32)
                z = z + zf_ref[span, :] if g else z - mean_one
                zf_ref[span, :] = z
                if g == groups - 1:
                    sums = moments(z, sums)
        if not last:
            share(mids(block + 1, 0), sums, index_of(block + 1, 0))

            def keep(t, carry):
                for g in range(groups):
                    updated(pl.multiple_of(t * chunk, 16), chunk, g, coefs[g], True)
                return carry

            lax.fori_loop(0, total_rows // chunk, keep, 0)


def last_kernel(pieces, x_ref, z3_ref, coef_ref, o_ref, y_ref, out_sem):
    slabs = x_ref.shape[0]
    pixels, images, channels = o_ref.shape
    part = pixels // pieces * images
    per = coef_ref.shape[1] // LANES
    done = slabs - per
    flat_ref = o_ref.reshape(pixels * images, channels)

    def old_copy(c):
        return pltpu.make_async_copy(
            x_ref.at[c], flat_ref.at[:, pl.ds(c * LANES, LANES)], out_sem.at[0]
        )

    def slab_copy(t, c):
        span = pl.ds(t * part, part)
        far = flat_ref.at[span, pl.ds((done + c) * LANES, LANES)]
        return pltpu.make_async_copy(y_ref.at[c, span], far, out_sem.at[1])

    for c in range(done):
        old_copy(c).start()

    def step(t, carry):
        span = pl.ds(pl.multiple_of(t * part, 16), part)
        for c in range(per):
            lanes = slice(c * LANES, (c + 1) * LANES)
            scale, offset = (coef_ref[pl.ds(i, 1), lanes] for i in range(2))
            z = z3_ref[done + c, span, :] * scale + offset
            y = z.astype(bf16) + x_ref[done + c, span, :]
            y_ref[c, span, :] = jnp.maximum(y, 0)
            slab_copy(t, c).start()
        return carry

    lax.fori_loop(0, pieces, step, 0)
    if done:
        old = x_ref.at[pl.ds(0, done)]
        pltpu.make_async_copy(old, old, out_sem.at[0]).wait()
    pltpu.make_async_copy(y_ref, y_ref, out_sem.at[1]).wait()


def local(mesh_rows, mesh_cols, images, w_reduce, w_spatial, w_expand, *params):
    held, side, _, channels = images.shape
    blocks, _, middle = w_reduce.shape
    devices = mesh_rows * mesh_cols
    count = float(held * side * side * devices)
    tiles = next(t for t in (TILES, 2, 1) if side % (2 * t) == 0)
    slabs = channels // LANES
    pixels = side * side
    loads_in = next(t for t in (4, 2, 1) if pixels * held % (16 * t) == 0)
    width = group_width(channels)
    groups = channels // width
    vmem = pl.BlockSpec(memory_space=pltpu.VMEM)
    anywhere = pl.BlockSpec(memory_space=pltpu.HBM)
    turned = images.transpose(1, 2, 0, 3).reshape(pixels, held, channels)
    taps = w_spatial.reshape(blocks, 9 * middle, middle)
    operands = [
        pltpu.with_memory_space_constraint(a, pltpu.HBM)
        for a in (turned, w_reduce, taps, w_expand, *params)
    ]
    x, z3, coef = pl.pallas_call(
        functools.partial(main_kernel, mesh_rows, mesh_cols, count, side, tiles, loads_in),
        out_shape=(
            jax.ShapeDtypeStruct((slabs, pixels * held, LANES), bf16),
            jax.ShapeDtypeStruct((slabs, pixels * held, LANES), f32),
            jax.ShapeDtypeStruct((2, width), f32),
        ),
        in_specs=[anywhere] * 12,
        out_specs=(vmem, vmem, vmem),
        scratch_shapes=[
            pltpu.VMEM((side // 2, 2, side * held, middle), f32),
            pltpu.VMEM((side + 2, side * held, 3 * middle), bf16),
            pltpu.VMEM((blocks, 12 * middle, 2 * middle), bf16),
            pltpu.VMEM((2 * blocks, devices, 2, middle), f32),
            pltpu.VMEM((blocks, groups, devices, 2, width), f32),
            pltpu.VMEM(w_reduce.shape, bf16),
            pltpu.VMEM((blocks, 2 * middle, channels), bf16),
            *(pltpu.VMEM(p.shape, f32) for p in params),
            pltpu.SemaphoreType.DMA((loads_in,)),
            pltpu.SemaphoreType.DMA((11,)),
            pltpu.SemaphoreType.DMA((blocks, 2)),
            pltpu.SemaphoreType.DMA(((2 + groups) * blocks,)),
            pltpu.SemaphoreType.DMA(((2 + groups) * blocks,)),
        ],
        compiler_params=pltpu.CompilerParams(
            collective_id=0, has_side_effects=True, vmem_limit_bytes=LIMIT * 1024 * 1024
        ),
        name="bottlenecks",
    )(*operands)
    pieces = side // 4 if side % 4 == 0 else 1
    out = pl.pallas_call(
        functools.partial(last_kernel, pieces),
        out_shape=jax.ShapeDtypeStruct((pixels, held, channels), bf16),
        in_specs=[vmem] * 3,
        out_specs=anywhere,
        scratch_shapes=[
            pltpu.VMEM((width // LANES, pixels * held, LANES), bf16),
            pltpu.SemaphoreType.DMA((2,)),
        ],
        compiler_params=pltpu.CompilerParams(vmem_limit_bytes=16 * 1024 * 1024),
        name="finish",
    )(x, z3, coef)
    return out.reshape(side, side, held, channels).transpose(2, 0, 1, 3)


TILES = 2
LIMIT = 32


def solution(mesh):
    spec = P(("row", "col"), None, None, None)
    return jax.shard_map(
        functools.partial(local, mesh.shape["row"], mesh.shape["col"]),
        mesh=mesh,
        in_specs=(spec,) + (P(),) * 11,
        out_specs=spec,
        check_vma=False,
    )
```

```python
import functools

import jax
import jax.numpy as jnp
from jax import lax
from jax.experimental import pallas as pl
from jax.experimental.pallas import tpu as pltpu
from jax.sharding import PartitionSpec as P

epsilon = 1e-05
ratio_max = 3.0
shift_max = 5.0
MESH = pl.DeviceIdType.MESH
LANES = 128
f32 = jnp.float32
bf16 = jnp.bfloat16


def coefficients(total, gain, bias, run_var, count):
    mean_offset = total[0:1] * (1.0 / count)
    variance = jnp.maximum(total[1:2] * (1.0 / count) - mean_offset * mean_offset, 0.0)
    inverse = lax.rsqrt(variance + epsilon)
    run_inverse = lax.rsqrt(run_var + epsilon)
    scale = gain * jnp.clip(run_inverse, inverse * (1.0 / ratio_max), inverse * ratio_max)
    shift = jnp.clip(mean_offset * run_inverse, -shift_max, shift_max)
    return scale, gain * shift + bias - mean_offset * scale


def flipped(index, bits):
    out, bit = index, 1
    while bit <= bits:
        if bits & bit:
            out = out + bit - 2 * bit * lax.rem(lax.div(index, bit), 2)
        bit *= 2
    return out


def tree_sum(parts):
    while len(parts) > 1:
        half = [a + b for a, b in zip(parts[0::2], parts[1::2])]
        parts = half + ([parts[-1]] if len(parts) % 2 else [])
    return parts[0]


def group_width(channels):
    return 2 * LANES if channels % (2 * LANES) == 0 else channels


def main_kernel(
    rows,
    cols,
    count,
    side,
    tiles,
    loads_in,
    img_ref,
    wr_hbm,
    ws_hbm,
    we_hbm,
    gm_hbm,
    bm_hbm,
    mm_hbm,
    vm_hbm,
    go_hbm,
    bo_hbm,
    mo_hbm,
    vo_hbm,
    x_ref,
    z3_ref,
    coef_ref,
    z_ref,
    hc_ref,
    w2_ref,
    mid_buf,
    out_buf,
    wr_ref,
    we_ref,
    gm_ref,
    bm_ref,
    mm_ref,
    vm_ref,
    go_ref,
    bo_ref,
    mo_ref,
    vo_ref,
    in_sem,
    par_sem,
    tap_sem,
    send_sem,
    recv_sem,
):
    devices = rows * cols
    pixels, images, channels = img_ref.shape
    blocks, _, middle = wr_ref.shape
    slabs = channels // LANES
    width = group_width(channels)
    groups = channels // width
    per = width // LANES
    line = side * images
    tall = side // tiles
    part = tall * line
    total_rows = pixels * images
    my_row, my_col = lax.axis_index("row"), lax.axis_index("col")
    me = my_row * cols + my_col
    flat_ref = img_ref.reshape(total_rows, channels)
    zf_ref = z_ref.reshape(total_rows, middle)
    piece = total_rows // loads_in
    chunk = next(16 * k for k in (14, 7, 4, 2, 1) if total_rows % (16 * k) == 0)

    def slab_copy(t, c):
        span = pl.ds(t * piece, piece)
        far = flat_ref.at[span, pl.ds(c * LANES, LANES)]
        return pltpu.make_async_copy(far, x_ref.at[c, span], in_sem.at[t])

    pairs = (
        (wr_hbm.at[0], wr_ref.at[0]), (mm_hbm, mm_ref), (we_hbm, we_ref.at[:, pl.ds(0, middle)]), (gm_hbm, gm_ref),
        (bm_hbm, bm_ref), (vm_hbm, vm_ref), (go_hbm, go_ref), (bo_hbm, bo_ref),
        (mo_hbm, mo_ref), (vo_hbm, vo_ref),
    )
    loads = [pltpu.make_async_copy(a, b, par_sem.at[i]) for i, (a, b) in enumerate(pairs)]
    if blocks > 1:
        rest = pl.ds(1, blocks - 1)
        loads.append(pltpu.make_async_copy(wr_hbm.at[rest], wr_ref.at[rest], par_sem.at[len(pairs)]))
    kernels = [
        pltpu.make_async_copy(
            ws_hbm.at[block],
            w2_ref.at[block, pl.ds(3 * i * middle, 9 * middle), pl.ds(i * middle, middle)],
            tap_sem.at[block, i],
        )
        for block in range(blocks)
        for i in range(2)
    ]
    barrier = pltpu.get_barrier_semaphore()

    def to_all(act):
        if devices <= 64:
            if rows & (rows - 1) == 0 and cols & (cols - 1) == 0:
                far_rows = [flipped(my_row, i) for i in range(rows)]
                far_cols = [flipped(my_col, i) for i in range(cols)]
            else:
                far_rows = [lax.rem(my_row + i, rows) for i in range(rows)]
                far_cols = [lax.rem(my_col + i, cols) for i in range(cols)]
            for j in range(cols - 1, -1, -1):
                for i in range(rows - 1, -1, -1):
                    if i or j:
                        act((far_rows[i], far_cols[j]))
        else:

            def step(i, c):
                other = lax.rem(me + i, devices)
                act((lax.div(other, cols), lax.rem(other, cols)))
                return c

            lax.fori_loop(1, devices, step, 0)

    for copy in loads[:2]:
        copy.start()
    to_all(
        lambda there: pl.semaphore_signal(
            barrier, inc=1, device_id=there, device_id_type=MESH
        )
    )

    for t in range(loads_in):
        for c in range(slabs):
            slab_copy(t, c).start()

    def slots(ref, index):
        others = ref.at[pl.ds(0, devices - 1)]
        return pltpu.make_async_remote_copy(
            src_ref=others,
            dst_ref=others,
            send_sem=send_sem.at[index],
            recv_sem=recv_sem.at[index],
            device_id=(lax.rem(my_row + 1, rows), my_col),
            device_id_type=MESH,
        )

    def share(ref, sums, index):
        for i in range(2):
            ref[me, pl.ds(i, 1), :] = jnp.sum(sums[i], axis=0, keepdims=True)
        if index == 0:
            pl.semaphore_wait(barrier, devices - 1)

        def send(there):
            pltpu.make_async_remote_copy(
                src_ref=ref.at[me],
                dst_ref=ref.at[me],
                send_sem=send_sem.at[index],
                recv_sem=recv_sem.at[index],
                device_id=there,
                device_id_type=MESH,
            ).start()

        to_all(send)

    def collect(ref, index):
        exchange = slots(ref, index)
        exchange.wait_send()
        exchange.wait_recv()
        if devices <= 64:
            return tree_sum([ref[d] for d in range(devices)])
        return jnp.sum(ref[...], axis=0)

    def moments(d, sums):
        d = d.reshape(-1, 8, d.shape[-1])
        return sums[0] + jnp.sum(d, axis=0), sums[1] + jnp.sum(d * d, axis=0)

    def zeros(c):
        return (jnp.zeros((8, c), f32), jnp.zeros((8, c), f32))

    for copy in loads[:2]:
        copy.wait()
    place = lax.broadcasted_iota(jnp.int32, (1, line, 1), 1)

    def updated(start, size, g, coef, keep):
        scale, offset = coef
        new = []
        for c in range(per):
            lanes = slice(c * LANES, (c + 1) * LANES)
            slab = g * per + c
            span = pl.ds(start, size)
            z = z3_ref[slab, span, :] * scale[:, lanes] + offset[:, lanes]
            y = jnp.maximum(z.astype(bf16) + x_ref[slab, span, :], 0)
            if keep:
                x_ref[slab, span, :] = y
            new.append(y)
        return new

    def halves(start, size):
        first = (size // 2 + 15) // 16 * 16
        return ((start, first), (start + first, size - first))

    per_block = 2 + groups

    def index_of(block, stage):
        return per_block * block + stage

    mids = lambda block, i: mid_buf.at[2 * block + i]
    outs = lambda block, g: out_buf.at[block, g]

    sums = zeros(middle)
    mean_one = mm_ref[0, pl.ds(0, 1), :]
    for t in range(loads_in):
        tile = x_ref.at[:, pl.ds(t * piece, piece)]
        pltpu.make_async_copy(tile, tile, in_sem.at[t]).wait()
        for start, size in halves(t * piece, piece):
            x = jnp.concatenate([x_ref[c, pl.ds(start, size), :] for c in range(slabs)], axis=1)
            z = jnp.dot(x, wr_ref[0], preferred_element_type=f32) - mean_one
            zf_ref[pl.ds(start, size), :] = z
            sums = moments(z, sums)
    share(mids(0, 0), sums, index_of(0, 0))
    for copy in loads[2:] + kernels:
        copy.start()
    hc_ref[0] = jnp.zeros((line, 3 * middle), bf16)
    hc_ref[side + 1] = jnp.zeros((line, 3 * middle), bf16)
    empty = jnp.zeros((3 * middle, middle), bf16)
    for block in range(blocks):
        w2_ref[block, pl.ds(9 * middle, 3 * middle), 0:middle] = empty
        w2_ref[block, pl.ds(0, 3 * middle), middle : 2 * middle] = empty
    for copy in loads[2:] + kernels:
        copy.wait()
    for block in range(blocks):
        left_over = -mo_ref[pl.ds(block, 1), :]
        digits = []
        for _ in range(3):
            digits.append(left_over.astype(bf16).astype(f32))
            left_over = left_over - digits[-1]
        place_in = lax.broadcasted_iota(jnp.int32, (middle, channels), 0)
        below = jnp.zeros((middle, channels), f32)
        for i, digit in enumerate(digits):
            below = jnp.where(place_in == i, digit, below)
        we_ref[block, pl.ds(middle, middle), :] = below.astype(bf16)
    ones = (lax.broadcasted_iota(jnp.int32, (part, LANES), 1) < 3).astype(f32).astype(bf16)

    for block in range(blocks):
        mean_two = mm_ref[block, pl.ds(1, 1), :]
        scale1, offset1 = coefficients(
            collect(mids(block, 0), index_of(block, 0)),
            gm_ref[block, pl.ds(0, 1), :], bm_ref[block, pl.ds(0, 1), :],
            vm_ref[block, pl.ds(0, 1), :], count,
        )

        for t in range(tiles):
            z = zf_ref[pl.ds(t * part, part), :]
            h = jnp.maximum(z * scale1 + offset1, 0.0)
            left = pltpu.roll(h, images, 0).reshape(tall, line, middle)
            right = pltpu.roll(h, part - images, 0).reshape(tall, line, middle)
            left = jnp.where(place >= images, left, 0.0)
            right = jnp.where(place < line - images, right, 0.0)
            taps = (left, h.reshape(tall, line, middle), right)
            for i, tap in enumerate(taps):
                lanes = slice(i * middle, (i + 1) * middle)
                hc_ref[pl.ds(t * tall + 1, tall), :, lanes] = tap.astype(bf16)

        sums = zeros(middle)
        for t in range(tiles):
            v = hc_ref[pl.ds(t * tall, tall + 2)].reshape(tall // 2 + 1, 2, line, 3 * middle)
            lhs = jnp.concatenate(
                [v[:-1, 0], v[:-1, 1], v[1:, 0], v[1:, 1]], axis=-1
            ).reshape(part // 2, 12 * middle)
            z = jnp.dot(lhs, w2_ref[block], preferred_element_type=f32)
            for i in range(2):
                half = z[:, i * middle : (i + 1) * middle] - mean_two
                z_ref[pl.ds(t * (tall // 2), tall // 2), i] = half.reshape(
                    tall // 2, line, middle
                )
                sums = moments(half, sums)
        share(mids(block, 1), sums, index_of(block, 1))
        scale2, offset2 = coefficients(
            collect(mids(block, 1), index_of(block, 1)),
            gm_ref[block, pl.ds(1, 1), :], bm_ref[block, pl.ds(1, 1), :],
            vm_ref[block, pl.ds(1, 1), :], count,
        )

        for g in range(groups):
            wide = slice(g * width, (g + 1) * width)
            sums = zeros(width)
            for t in range(tiles):
                span = pl.ds(t * part, part)
                h = zf_ref[span, :]
                if g == 0:
                    h = jnp.maximum(h * scale2 + offset2, 0.0)
                    zf_ref[span, :] = h
                h = h.astype(bf16)
                lhs = jnp.concatenate([h, ones], axis=1)
                z = jnp.dot(lhs, we_ref[block, :, wide], preferred_element_type=f32)
                for c in range(per):
                    z3_ref[g * per + c, span, :] = z[:, c * LANES : (c + 1) * LANES]
                sums = moments(z, sums)
            share(outs(block, g), sums, index_of(block, 2 + g))

        last = block == blocks - 1
        if not last:
            mean_one = mm_ref[block + 1, pl.ds(0, 1), :]
            sums = zeros(middle)
        coefs = []
        for g in range(groups):
            wide = slice(g * width, (g + 1) * width)
            coef = coefficients(
                collect(outs(block, g), index_of(block, 2 + g)),
                go_ref[pl.ds(block, 1), wide], bo_ref[pl.ds(block, 1), wide],
                vo_ref[pl.ds(block, 1), wide], count,
            )
            coefs.append(coef)
            if last and g == groups - 1:
                for i in range(2):
                    coef_ref[pl.ds(i, 1), :] = coef[i]
                break
            for t in range(tiles):
                y = updated(t * part, part, g, coef, last)
                if last:
                    continue
                span = pl.ds(t * part, part)
                y = jnp.concatenate(y, axis=1)
                z = jnp.dot(y, wr_ref[block + 1, wide, :], preferred_element_type=f32)
                z = z + zf_ref[span, :] if g else z - mean_one
                zf_ref[span, :] = z
                if g == groups - 1:
                    sums = moments(z, sums)
        if not last:
            share(mids(block + 1, 0), sums, index_of(block + 1, 0))

            def keep(t, carry):
                for g in range(groups):
                    updated(pl.multiple_of(t * chunk, 16), chunk, g, coefs[g], True)
                return carry

            lax.fori_loop(0, total_rows // chunk, keep, 0)


def last_kernel(pieces, x_ref, z3_ref, coef_ref, o_ref, y_ref, out_sem):
    slabs = x_ref.shape[0]
    pixels, images, channels = o_ref.shape
    part = pixels // pieces * images
    per = coef_ref.shape[1] // LANES
    done = slabs - per
    flat_ref = o_ref.reshape(pixels * images, channels)

    def old_copy(c):
        return pltpu.make_async_copy(
            x_ref.at[c], flat_ref.at[:, pl.ds(c * LANES, LANES)], out_sem.at[0]
        )

    def slab_copy(t, c):
        span = pl.ds(t * part, part)
        far = flat_ref.at[span, pl.ds((done + c) * LANES, LANES)]
        return pltpu.make_async_copy(y_ref.at[c, span], far, out_sem.at[1])

    for c in range(done):
        old_copy(c).start()

    def step(t, carry):
        span = pl.ds(pl.multiple_of(t * part, 16), part)
        for c in range(per):
            lanes = slice(c * LANES, (c + 1) * LANES)
            scale, offset = (coef_ref[pl.ds(i, 1), lanes] for i in range(2))
            z = z3_ref[done + c, span, :] * scale + offset
            y = z.astype(bf16) + x_ref[done + c, span, :]
            y_ref[c, span, :] = jnp.maximum(y, 0)
            slab_copy(t, c).start()
        return carry

    lax.fori_loop(0, pieces, step, 0)
    if done:
        old = x_ref.at[pl.ds(0, done)]
        pltpu.make_async_copy(old, old, out_sem.at[0]).wait()
    pltpu.make_async_copy(y_ref, y_ref, out_sem.at[1]).wait()


def local(mesh_rows, mesh_cols, images, w_reduce, w_spatial, w_expand, *params):
    held, side, _, channels = images.shape
    blocks, _, middle = w_reduce.shape
    devices = mesh_rows * mesh_cols
    count = float(held * side * side * devices)
    tiles = next(t for t in (TILES, 2, 1) if side % (2 * t) == 0)
    slabs = channels // LANES
    pixels = side * side
    loads_in = next(t for t in (4, 2, 1) if pixels * held % (16 * t) == 0)
    width = group_width(channels)
    groups = channels // width
    vmem = pl.BlockSpec(memory_space=pltpu.VMEM)
    anywhere = pl.BlockSpec(memory_space=pltpu.HBM)
    turned = images.transpose(1, 2, 0, 3).reshape(pixels, held, channels)
    taps = w_spatial.reshape(blocks, 9 * middle, middle)
    operands = [
        pltpu.with_memory_space_constraint(a, pltpu.HBM)
        for a in (turned, w_reduce, taps, w_expand, *params)
    ]
    x, z3, coef = pl.pallas_call(
        functools.partial(main_kernel, mesh_rows, mesh_cols, count, side, tiles, loads_in),
        out_shape=(
            jax.ShapeDtypeStruct((slabs, pixels * held, LANES), bf16),
            jax.ShapeDtypeStruct((slabs, pixels * held, LANES), f32),
            jax.ShapeDtypeStruct((2, width), f32),
        ),
        in_specs=[anywhere] * 12,
        out_specs=(vmem, vmem, vmem),
        scratch_shapes=[
            pltpu.VMEM((side // 2, 2, side * held, middle), f32),
            pltpu.VMEM((side + 2, side * held, 3 * middle), bf16),
            pltpu.VMEM((blocks, 12 * middle, 2 * middle), bf16),
            pltpu.VMEM((2 * blocks, devices, 2, middle), f32),
            pltpu.VMEM((blocks, groups, devices, 2, width), f32),
            pltpu.VMEM(w_reduce.shape, bf16),
            pltpu.VMEM((blocks, 2 * middle, channels), bf16),
            *(pltpu.VMEM(p.shape, f32) for p in params),
            pltpu.SemaphoreType.DMA((loads_in,)),
            pltpu.SemaphoreType.DMA((11,)),
            pltpu.SemaphoreType.DMA((blocks, 2)),
            pltpu.SemaphoreType.DMA(((2 + groups) * blocks,)),
            pltpu.SemaphoreType.DMA(((2 + groups) * blocks,)),
        ],
        compiler_params=pltpu.CompilerParams(
            collective_id=0, has_side_effects=True, vmem_limit_bytes=LIMIT * 1024 * 1024
        ),
        name="bottlenecks",
    )(*operands)
    pieces = side // 4 if side % 4 == 0 else 1
    out = pl.pallas_call(
        functools.partial(last_kernel, pieces),
        out_shape=jax.ShapeDtypeStruct((pixels, held, channels), bf16),
        in_specs=[vmem] * 3,
        out_specs=anywhere,
        scratch_shapes=[
            pltpu.VMEM((width // LANES, pixels * held, LANES), bf16),
            pltpu.SemaphoreType.DMA((2,)),
        ],
        compiler_params=pltpu.CompilerParams(vmem_limit_bytes=16 * 1024 * 1024),
        name="finish",
    )(x, z3, coef)
    return out.reshape(side, side, held, channels).transpose(2, 0, 1, 3)


TILES = 2
LIMIT = 32


def solution(mesh):
    spec = P(("row", "col"), None, None, None)
    return jax.shard_map(
        functools.partial(local, mesh.shape["row"], mesh.shape["col"]),
        mesh=mesh,
        in_specs=(spec,) + (P(),) * 11,
        out_specs=spec,
        check_vma=False,
    )
```
